128 devices in a mesh: row: 32 (over z, x, core), col: 4 (over y).
Axes of the slice: x: 4, y: 4, z: 4, core: 2. Of those that a mesh axis runs over, the one named last changes fastest.
Arguments:
- spikes: int32 [10, 16384], P(None, ('row', 'col')), may hold values 0 or 1
- stp_init: float32 [2, 16384], P(None, ('row', 'col')), may hold values from 0.2 to 1
- trace_init: float32 [3, 16384], P(None, ('row', 'col')), may hold values from 0 to 1.5
- weights: float32 [32, 4, 256, 128, 128], P('row', 'col'), may hold values from 0 to 1
- block_pre: int32 [32, 4, 256], P('row', 'col'), may hold values from 0 to 31
- block_post: int32 [32, 4, 256], P('row', 'col'), may hold values from 0 to 3
- block_count: int32 [32, 4], P('row', 'col'), may hold values from 1 to 255, as said below
Outputs:
- new_weights: float32 [32, 4, 128, 128, 128], P('row', 'col')
- synaptic: float32 [10, 16384], P(None, ('row', 'col'))
The draws below stay inside these ranges and needn't reach their ends.
Inputs may be any that keep to these rules, and one draw needn't show every extreme that they name: block_count[r, c] + block_count[(r + 16) mod 32, c] = 256; some device uses 2 * 128 - 1 slots in every draw.
All inputs are finite; a program needn't handle non-finite values. No bound on the sum of `spikes` on one device may be relied on, other than what follows from the above.
Results may differ from the reference program's by a relative error of at most 0.0003.
Values sent between devices are 32-bit elements; how exact they have to be, the bound alone decides.
A program may use at most 128 MiB of HBM per device.

```python
import math
import jax
import jax.numpy as jnp
import numpy as np
from jax import lax

GRP = 128
BLK_DEV = 128
STEPS = 10
SLOTS = 256
NEURONS = 16384
N_ROW = 32
N_COL = 4


def draw_block_count(key, part):
    half_rows = N_ROW // 2
    keys = jax.random.split(key, 5)
    first = jax.random.randint(keys[0], (half_rows, N_COL), 0, BLK_DEV)
    second = jax.random.randint(keys[1], (half_rows, N_COL), 0, BLK_DEV)
    spread_size = first * second // max(BLK_DEV - 1, 1)
    chosen_row = jax.random.randint(keys[2], (), 0, half_rows)
    chosen_col = jax.random.randint(keys[3], (), 0, N_COL)
    forced = (jnp.arange(half_rows)[:, None] == chosen_row) & (jnp.arange(N_COL)[None, :] == chosen_col)
    spread_size = jnp.where(forced, BLK_DEV - 1, spread_size)
    flips = jax.random.randint(keys[4], (half_rows, N_COL), 0, 2) * 2 - 1
    offset = spread_size * flips
    return jnp.concatenate([BLK_DEV + offset, BLK_DEV - offset], axis=0).astype(jnp.int32)


def touch_ends(entries, rng, smallest, largest):
    spot = [jax.random.randint(jax.random.fold_in(rng, axis), (), 0, length) for axis, length in enumerate(entries.shape)]
    main_axis = entries.shape.index(max(entries.shape))
    next_to = spot[:main_axis] + [(spot[main_axis] + 1) % entries.shape[main_axis]] + spot[main_axis + 1:]
    return entries.at[tuple(spot)].set(smallest).at[tuple(next_to)].set(largest)


def steps_of(stream_key, shape, shards, low, top_value):
    def one(dim, blocks):
        steps = jax.random.uniform(jax.random.fold_in(jax.random.fold_in(stream_key, 6), dim), (blocks,), jnp.float32, low / len(shards), top_value / len(shards))
        return jnp.repeat(jnp.exp(steps), shape[dim] // blocks).reshape((-1,) + (1,) * (len(shape) - dim - 1))

    loudness = one(*shards[0])
    for cut in shards[1:]:
        loudness = loudness * one(*cut)
    return loudness


def rank_table(amount, lean):
    weights = [(1 << 20) // math.isqrt(grade ** lean) + 1 for grade in range(1, amount + 1)]
    spread = 1 + sum(weights) // (1 << 30)
    return np.cumsum(np.array([max(1, weight // spread) for weight in weights]))


def skewed_ids(stream_key, extent, count, slope):
    grid = rank_table(count, slope)
    lot = jax.random.randint(jax.random.fold_in(stream_key, 1), extent, 0, int(grid[count - 1]))
    rank = jnp.searchsorted(jnp.asarray(grid, jnp.int32), lot, side="right")
    return jax.random.permutation(jax.random.fold_in(stream_key, 2), count)[rank].astype(jnp.int32)


def setup_inputs(seed: int = 0) -> dict:
    key_of = jax.random.split(jax.random.key(seed), 8)
    spikes = touch_ends((jax.random.randint(key_of[0], (STEPS, NEURONS), 0, 4) < 1).astype(jnp.int32), jax.random.fold_in(key_of[0], 1), 0, 1)
    stp_init = jnp.clip(0.2 + 0.8 * jax.random.uniform(key_of[1], (2, NEURONS), jnp.float32) ** steps_of(key_of[1], (2, NEURONS), ((1, 128),), -0.2, 0.2), 0.2, 1.0)
    trace_init = jnp.clip(1.5 * jax.random.uniform(key_of[2], (3, NEURONS), jnp.float32) ** steps_of(key_of[2], (3, NEURONS), ((1, 128),), -0.2, 0.2), 0.0, 1.5)
    weights = jnp.clip(1.0 * jax.random.uniform(key_of[3], (N_ROW, N_COL, SLOTS, GRP, GRP), jnp.float32) ** steps_of(key_of[3], (N_ROW, N_COL, SLOTS, GRP, GRP), ((0, 32), (1, 4)), -0.2, 0.2), 0.0, 1.0)
    block_pre = touch_ends(skewed_ids(key_of[4], (N_ROW, N_COL, SLOTS), N_ROW, 2), jax.random.fold_in(key_of[4], 3), 0, N_ROW - 1).astype(jnp.int32)
    block_post = touch_ends(jax.random.randint(key_of[5], (N_ROW, N_COL, SLOTS), 0, N_COL), jax.random.fold_in(key_of[5], 1), 0, N_COL - 1).astype(jnp.int32)
    block_count = draw_block_count(jax.random.fold_in(key_of[7], 71), 0)
    return dict(spikes=spikes, stp_init=stp_init, trace_init=trace_init, weights=weights, block_pre=block_pre, block_post=block_post, block_count=block_count)


HIGHEST = lax.Precision.HIGHEST
BASE_USE = 0.25
USE_DECAY = 0.98
SUPPLY_RATE = 0.005
PLUS_DECAY = math.exp(-1.0 / 16.8)
MINUS_DECAY = math.exp(-1.0 / 33.7)
SLOW_DECAY = math.exp(-1.0 / 114.0)
SYN_DECAY = math.exp(-1.0 / 5.0)
PAIR_UP = 1.0
TRIPLET_UP = 0.8
PAIR_DOWN = 0.9
LEARN_RATE = 0.02
WEIGHT_MAX = 1.0
INHIB_GAIN = 4.0

def neuron_traces(spikes, stp_init, trace_init):
    fired = spikes.astype(jnp.float32)

    def advance(carry, fired_now):
        use_level, supply, pre_fast, post_fast, post_slow = carry
        use_level = BASE_USE + (use_level - BASE_USE) * USE_DECAY
        use_level = use_level + fired_now * BASE_USE * (1.0 - use_level)
        release = fired_now * use_level * supply
        supply = supply + SUPPLY_RATE * (1.0 - supply) - release
        pre_fast = pre_fast * PLUS_DECAY + fired_now
        potent = fired_now * (PAIR_UP + TRIPLET_UP * post_slow)
        depress = PAIR_DOWN * post_fast
        post_fast = post_fast * MINUS_DECAY + fired_now
        post_slow = post_slow * SLOW_DECAY + fired_now
        return ((use_level, supply, pre_fast, post_fast, post_slow), (release, pre_fast, potent, depress))
    start = (stp_init[0], stp_init[1], trace_init[0], trace_init[1], trace_init[2])
    _, results = lax.scan(advance, start, fired)
    return results

def block_work(weights, pre_blocks, post_blocks, polarity):
    release = pre_blocks[:, 0]
    pre_fast = pre_blocks[:, 1]
    potent = post_blocks[:, 0]
    depress = post_blocks[:, 1]
    driven = release * polarity
    current = jnp.einsum('nij,nsj->nsi', weights, driven, precision=HIGHEST)
    post_terms = jnp.concatenate([potent, -depress], axis=1)
    pre_terms = jnp.concatenate([pre_fast, release], axis=1)
    change = jnp.einsum('nki,nkj->nij', post_terms, pre_terms, precision=HIGHEST)
    return (current, jnp.clip(weights + LEARN_RATE * change, 0.0, WEIGHT_MAX))

def arrange(own_updated, partner_upper, filled):
    half_slots = partner_upper.shape[0]
    places = jnp.arange(half_slots, dtype=jnp.int32)
    picked = jnp.clip(places - filled, 0, half_slots - 1).astype(jnp.int32)
    return jnp.where((places < filled)[:, None, None], own_updated[:half_slots], jnp.take(partner_upper, picked, axis=0))

def filtered(drive, gain):

    def advance(state, current):
        state = state * SYN_DECAY + gain * current
        return (state, state)
    _, result = lax.scan(advance, jnp.zeros_like(drive[0]), drive)
    return result

def reference(spikes, stp_init, trace_init, weights, block_pre, block_post, block_count):
    polarity = jnp.where(jnp.arange(GRP) % 5 == 4, -INHIB_GAIN, 1.0).astype(jnp.float32)
    release, pre_fast, potent, depress = neuron_traces(spikes, stp_init, trace_init)
    packed = jnp.stack([release, pre_fast, potent, depress]).reshape(4, STEPS, N_ROW, N_COL, GRP)
    pre_tables = jnp.transpose(packed[0:2], (3, 2, 0, 1, 4))
    post_all = packed[2:4]
    half_rows = N_ROW // 2

    def row_work(row_index, weights_row, pre_row, post_row, count_row):
        post_table = jnp.transpose(lax.dynamic_index_in_dim(post_all, row_index, 2, keepdims=False), (2, 0, 1, 3))

        def per_col(weights_col, pre_col, post_col, filled, pre_table):
            current, updated = block_work(weights_col, jnp.take(pre_table, pre_col, axis=0), jnp.take(post_table, post_col, axis=0), polarity)
            usable = jnp.arange(weights_col.shape[0], dtype=jnp.int32) < filled
            onehot = ((post_col[:, None] == jnp.arange(N_COL, dtype=jnp.int32)[None, :]) & usable[:, None]).astype(jnp.float32)
            return (jnp.einsum('nq,nsi->qsi', onehot, current, precision=HIGHEST), updated)
        partial_value, updated = jax.vmap(per_col)(weights_row, pre_row, post_row, count_row, pre_tables)
        return (lax.optimization_barrier(jnp.sum(partial_value, axis=0)), updated)

    def pair_work(items):
        row_low, low_weights, high_weights, low_pre, high_pre, low_post, high_post, low_count, high_count = items
        cur_low, upd_low = row_work(row_low, low_weights, low_pre, low_post, low_count)
        cur_high, upd_high = row_work(row_low + half_rows, high_weights, high_pre, high_post, high_count)
        new_low = jax.vmap(arrange)(upd_low, upd_high[:, BLK_DEV:], low_count)
        new_high = jax.vmap(arrange)(upd_high, upd_low[:, BLK_DEV:], high_count)
        return (cur_low, cur_high, new_low, new_high)
    cur_low, cur_high, new_low, new_high = lax.map(pair_work, (jnp.arange(half_rows, dtype=jnp.int32), weights[:half_rows], weights[half_rows:], block_pre[:half_rows], block_pre[half_rows:], block_post[:half_rows], block_post[half_rows:], block_count[:half_rows], block_count[half_rows:]))
    new_weights = jnp.concatenate([new_low, new_high], axis=0)
    drive = jnp.concatenate([cur_low, cur_high], axis=0)
    drive = jnp.transpose(drive, (2, 0, 1, 3)).reshape(STEPS, N_ROW * N_COL * GRP)
    synaptic = filtered(drive, 1.0 / math.sqrt(GRP * BLK_DEV))
    return (new_weights, synaptic)
```

```python
import functools
import math

import jax
import jax.numpy as jnp
from jax import lax
from jax.experimental import pallas as pl
from jax.experimental.pallas import tpu as pltpu
from jax.sharding import PartitionSpec as P

BASE_USE = 0.25
USE_DECAY = 0.98
SUPPLY_RATE = 0.005
PLUS_DECAY = math.exp(-1.0 / 16.8)
MINUS_DECAY = math.exp(-1.0 / 33.7)
SLOW_DECAY = math.exp(-1.0 / 114.0)
SYN_DECAY = math.exp(-1.0 / 5.0)
PAIR_UP = 1.0
TRIPLET_UP = 0.8
PAIR_DOWN = 0.9
LEARN_RATE = 0.02
WEIGHT_MAX = 1.0
INHIB_GAIN = 4.0

G = 128
HALF = 128
STEPS = 10
ROWS = 32
COLS = 4
MESH = pl.DeviceIdType.MESH
F32 = jnp.float32
I32 = jnp.int32
BF16 = jnp.bfloat16

E = 7
ES = 32
FAR = 8 * E
SLOTS_S = FAR + ES
M0 = 12
M1 = 20
RUNGS = (44, 48, 54, 62)
ITERS = 8
STEP_W = 10.0
ORDER = (1, 2, 3, 4, 5, 6, 7, 8, 0)
INVERSE = (0, 3, 4, 1, 2, 7, 8, 5, 6)
BASE = tuple([FAR] + [(k - 1) * E for k in range(1, 9)])
CAP = tuple([ES] + [E] * 8)
VMEM_LIMIT = 60 * 1024 * 1024
ANY = pl.BlockSpec(memory_space=pl.ANY)
SMEM = pl.BlockSpec(memory_space=pltpu.SMEM)
VMEM = pl.BlockSpec(memory_space=pltpu.VMEM)


def place():
    row, col = lax.axis_index("row"), lax.axis_index("col")
    return row, col


def at(row, col):
    return {"row": row, "col": col}


def flip_core(row):
    return row + 1 - 2 * lax.rem(row, 2)


def across(row):
    return lax.rem(row + ROWS // 2, ROWS)


def shift_x(row, step):
    within = lax.rem(row, 8)
    return row - within + lax.rem(within + 2 * step + 8, 8)


def neighbour(k, row, col):
    if k == 0:
        return at(flip_core(row), col)
    which, other = (k - 1) // 2, (k - 1) % 2
    if which < 2:
        row = shift_x(row, 1 if which == 0 else -1)
    else:
        col = lax.rem(col + (1 if which == 2 else COLS - 1), COLS)
    return at(flip_core(row) if other else row, col)


def greet(peers):
    barrier = pltpu.get_barrier_semaphore()
    for peer in peers:
        pl.semaphore_signal(barrier, inc=1, device_id=peer, device_id_type=MESH)
    pl.semaphore_wait(barrier, len(peers))


def send(src, dst, send_sem, recv_sem, peer):
    return pltpu.make_async_remote_copy(
        src_ref=src, dst_ref=dst, send_sem=send_sem, recv_sem=recv_sem, device_id=peer, device_id_type=MESH
    )


def tables_kernel(pack, idx, tab, rtab, ptab, pidx, cnt, s1, r1, s2, r2, s3, r3, s4, r4):
    row, col = place()
    far = across(row)
    barrier = pltpu.get_barrier_semaphore()

    @pl.loop(1, ROWS)
    def _(d):
        peer = at(lax.rem(row + d, ROWS), col)
        pl.semaphore_signal(barrier, inc=1, device_id=peer, device_id_type=MESH)

    for d in range(1, COLS):
        c = lax.rem(col + d, COLS)
        pl.semaphore_signal(barrier, inc=1, device_id=at(row, c), device_id_type=MESH)
        pl.semaphore_signal(barrier, inc=1, device_id=at(far, c), device_id_type=MESH)
    pl.semaphore_wait(barrier, ROWS - 1 + 2 * (COLS - 1))

    @pl.loop(1, ROWS)
    def _(d):
        peer = at(lax.rem(row + d, ROWS), col)
        send(pack, tab.at[row], s1.at[d], r1.at[row], peer).start()

    small = []
    for d in range(1, COLS):
        c = lax.rem(col + d, COLS)
        small.append(send(pack, rtab.at[col], s2.at[d], r2.at[col], at(row, c)))
    for d in range(COLS):
        c = lax.rem(col + d, COLS)
        small.append(send(pack, ptab.at[col], s3.at[d], r3.at[col], at(far, c)))
    small.append(send(idx, pidx, s4.at[0], r4.at[0], at(far, col)))
    for copy in small:
        copy.start()
    tab[row] = pack[...]
    rtab[col] = pack[...]

    @pl.loop(1, ROWS)
    def _(d):
        source = lax.rem(row + d, ROWS)
        send(pack, tab.at[source], s1.at[d], r1.at[source], at(source, col)).wait()

    cnt[col] = tab[:, 15, :]
    counts = []
    for d in range(1, COLS):
        c = lax.rem(col + d, COLS)
        counts.append(send(cnt.at[col], cnt.at[col], s4.at[d], r4.at[1 + col], at(row, c)))
    for copy in counts:
        copy.start()
    for d in range(1, COLS):
        c = lax.rem(col + d, COLS)
        send(pack, rtab.at[c], s2.at[d], r2.at[c], at(row, c)).wait()
    for d in range(COLS):
        c = lax.rem(col + d, COLS)
        send(pack, ptab.at[c], s3.at[d], r3.at[c], at(far, c)).wait()
    small[-1].wait()
    for d in range(1, COLS):
        c = lax.rem(col + d, COLS)
        send(cnt.at[c], cnt.at[c], s4.at[d], r4.at[1 + c], at(row, c)).wait()


def exchange_tables(pack, idx):
    dma = pltpu.SemaphoreType.DMA
    return pl.pallas_call(
        tables_kernel,
        out_shape=(
            jax.ShapeDtypeStruct((ROWS, 16, G), F32),
            jax.ShapeDtypeStruct((COLS, 16, G), F32),
            jax.ShapeDtypeStruct((COLS, 16, G), F32),
            jax.ShapeDtypeStruct((8, G), I32),
            jax.ShapeDtypeStruct((COLS, ROWS, G), F32),
        ),
        in_specs=[VMEM, VMEM],
        out_specs=(VMEM,) * 5,
        scratch_shapes=[
            dma((ROWS,)), dma((ROWS,)), dma((COLS,)), dma((COLS,)),
            dma((COLS,)), dma((COLS,)), dma((COLS,)), dma((COLS + 1,)),
        ],
        compiler_params=pltpu.CompilerParams(collective_id=0, has_side_effects=True),
        name="tables",
    )(pack, idx)


def plan_kernel(cnt, tables, rung):
    row, col = place()
    shape = (8, G)
    lane = lax.broadcasted_iota(I32, shape, 1)
    sub = lax.broadcasted_iota(I32, (ROWS, G), 0)
    lane_t = lax.broadcasted_iota(I32, (ROWS, G), 1)
    total = jnp.zeros((1, G), F32)
    for c in range(COLS):
        total = total + jnp.sum(jnp.where(lane_t == sub + c * ROWS, cnt[c], 0.0), axis=0, keepdims=True)
    count = jnp.broadcast_to(total, shape)
    surplus = jnp.maximum(count - HALF, 0.0)
    core = lax.rem(lane, 2)
    x_at = lax.rem(lane, 8) // 2
    z_hi = lax.rem(lane, 32) // 16

    def roll(value, by):
        return pltpu.roll(value, by % G, 1)

    def from_sibling(v):
        return jnp.where(core == 0, roll(v, -1), roll(v, 1))

    def seen(v):
        same = (
            jnp.where(x_at == 3, roll(v, 6), roll(v, -2)),
            jnp.where(x_at == 0, roll(v, -6), roll(v, 2)),
            roll(v, -ROWS),
            roll(v, ROWS),
        )
        out = [from_sibling(v)]
        for value in same:
            out += [value, from_sibling(value)]
        return out

    outs = [jnp.zeros(shape, F32)] * 9
    ins = [jnp.zeros(shape, F32)] * 9
    for _ in range(ITERS):
        load = surplus
        for k in range(9):
            load = load - outs[k] + ins[k]
        near = seen(load)
        for k in range(9):
            gap = (load - near[k]) * (1.0 / STEP_W)
            outs[k] = jnp.clip(outs[k] + gap, 0.0, float(CAP[k]))
        spent = functools.reduce(jnp.add, outs)
        scale = jnp.minimum(1.0, surplus / jnp.maximum(spent, 1e-6))
        outs = [v * scale for v in outs]
        moved = [None] * 9
        moved[0] = from_sibling(outs[0])
        back = (
            lambda v: jnp.where(x_at == 3, roll(v, 6), roll(v, -2)),
            lambda v: jnp.where(x_at == 0, roll(v, -6), roll(v, 2)),
            lambda v: roll(v, -ROWS),
            lambda v: roll(v, ROWS),
        )
        for k in range(1, 9):
            value = back[(k - 1) // 2](outs[INVERSE[k]])
            moved[k] = from_sibling(value) if (k - 1) % 2 else value
        ins = moved
    give = [jnp.minimum(jnp.floor(v + 0.5), float(CAP[k])) for k, v in enumerate(outs)]
    over = jnp.maximum(functools.reduce(jnp.add, give) - surplus, 0.0)
    for k in range(9):
        cut = jnp.minimum(give[k], over)
        give[k] = give[k] - cut
        over = over - cut
    take = [None] * 9
    take[0] = from_sibling(give[0])
    for k in range(1, 9):
        value = back[(k - 1) // 2](give[INVERSE[k]])
        take[k] = from_sibling(value) if (k - 1) % 2 else value
    own = surplus - functools.reduce(jnp.add, give)
    far_in = functools.reduce(jnp.add, take[1:])
    need = jnp.maximum(own, float(M0)) + far_in + take[0]
    worst = jnp.max(need)
    worst_far = jnp.max(far_in)
    picked = jnp.int32(0)
    for size in RUNGS:
        picked = picked + jnp.where(worst > float(size), 1, 0)
    picked = jnp.where(worst_far > float(M1), len(RUNGS), picked)
    full = picked == len(RUNGS)
    rung[0] = picked

    me = col * ROWS + row
    mate = col * ROWS + across(row)

    def of(v, who):
        return jnp.max(jnp.where(lane == who, v, -1.0), axis=1, keepdims=True).astype(I32)[:1]

    give_me = [of(v, me) for v in give]
    give_mate = [of(v, mate) for v in give]
    take_me = [of(v, me) for v in take]
    take_mate = [of(v, mate) for v in take]
    own_me, own_mate = of(own, me), of(own, mate)
    held = of(count, me)
    slot = lax.broadcasted_iota(I32, (1, G), 1)

    def table(i, value, top):
        tables[pl.ds(i, 1), :] = jnp.clip(value, 0, top)

    spread = jnp.zeros((1, G), I32)
    gather = jnp.zeros((1, G), I32)
    before_give, before_take = own_me, jnp.zeros((1, 1), I32)
    for k in ORDER:
        here = (slot >= BASE[k]) & (slot < BASE[k] + CAP[k])
        spread = jnp.where(here, slot - BASE[k] + before_give, spread)
        gather = jnp.where(here, slot - BASE[k] + before_take, gather)
        before_give = before_give + give_me[k]
        before_take = before_take + take_mate[k]
    table(0, spread, HALF - 1)
    turn = slot - M0
    ahead = jnp.zeros((1, 1), I32)
    imported = jnp.zeros((1, G), I32)
    is_import = jnp.zeros((1, G), I32)
    for k in ORDER:
        here = (turn >= ahead) & (turn < ahead + take_me[k])
        imported = jnp.where(here, BASE[k] + turn - ahead, imported)
        is_import = jnp.where(here, 1, is_import)
        ahead = ahead + take_me[k]
    table(1, M0 + turn - ahead, HALF - 1)
    table(2, imported, SLOTS_S - 1)
    table(3, is_import, 1)
    table(4, gather, HALF - 1)
    j = slot - held
    spot = jnp.where(j < M0, j, j + functools.reduce(jnp.add, take_mate))
    before = own_mate
    for k in ORDER:
        here = (j >= before) & (j < before + give_mate[k])
        spot = jnp.where(here, HALF + BASE[k] + j - before, spot)
        before = before + give_mate[k]
    spot = jnp.where(full, j, spot)
    table(5, jnp.where(j < 0, 0, spot), HALF + SLOTS_S - 1)
    table(6, jnp.where(j < 0, 0, 1), 1)
    table(7, j, HALF - 1)


def make_plan(cnt):
    return pl.pallas_call(
        plan_kernel,
        out_shape=(jax.ShapeDtypeStruct((8, G), I32), jax.ShapeDtypeStruct((1,), I32)),
        in_specs=[VMEM],
        out_specs=(VMEM, SMEM),
        name="plan",
    )(cnt)


def move_kernel(size, tables, weights, staged, up, spread, imports, z1, z2, got1, got2, back, ls, ss, rs, zs, zr, gs, gr):
    row, col = place()
    mate = at(across(row), col)
    peers = [neighbour(k, row, col) for k in range(9)]
    m2 = size - M0 - M1
    load = pltpu.make_async_copy(weights.at[pl.ds(HALF, HALF)], up, ls.at[0])
    load.start()
    greet(peers + [mate])
    load.wait()
    first = send(up.at[pl.ds(0, M0)], staged.at[pl.ds(0, M0)], zs.at[0], zr.at[0], mate)
    first.start()

    spreads = [
        send(spread.at[pl.ds(BASE[k], CAP[k])], imports.at[pl.ds(BASE[INVERSE[k]], CAP[k])], ss.at[k], rs.at[INVERSE[k]], peers[k])
        for k in range(9)
    ]
    for k in ORDER:

        @pl.loop(BASE[k], BASE[k] + CAP[k])
        def _(i):
            spread[i] = up[tables[0, i]]

        spreads[k].start()
    for k in range(9):
        send(spread.at[pl.ds(BASE[k], CAP[k])], imports.at[pl.ds(BASE[k], CAP[k])], ss.at[k], rs.at[k], peers[k]).wait_recv()

    def fill(target, start, count):
        @pl.loop(0, count)
        def _(i):
            at_slot = start + i
            target[i] = jnp.where(tables[3, at_slot] == 1, imports[tables[2, at_slot]], up[tables[1, at_slot]])

    second = send(z1, got1, zs.at[1], zr.at[1], mate)
    third = send(z2, got2, zs.at[2], zr.at[2], mate)
    fill(z1, M0, M1)
    second.start()
    fill(z2, M0 + M1, m2)
    third.start()

    gathers = [
        send(back.at[pl.ds(BASE[k], CAP[k])], staged.at[pl.ds(HALF + BASE[INVERSE[k]], CAP[k])], gs.at[k], gr.at[INVERSE[k]], peers[k])
        for k in range(9)
    ]
    second.wait_recv()
    for k in range(1, 9):

        @pl.loop(BASE[k], BASE[k] + CAP[k])
        def _(i):
            back[i] = got1[jnp.minimum(tables[4, i], M1 - 1)]

        gathers[k].start()
    out1 = pltpu.make_async_copy(got1, staged.at[pl.ds(M0, M1)], ls.at[1])
    out1.start()
    third.wait_recv()
    out2 = pltpu.make_async_copy(got2, staged.at[pl.ds(M0 + M1, m2)], ls.at[2])
    out2.start()

    @pl.loop(BASE[0], BASE[0] + ES)
    def _(i):
        t = tables[4, i]
        back[i] = jnp.where(t < M1, got1[jnp.minimum(t, M1 - 1)], got2[jnp.clip(t - M1, 0, m2 - 1)])

    gathers[0].start()
    out1.wait()
    out2.wait()
    first.wait()
    second.wait_send()
    third.wait_send()
    for k in range(9):
        spreads[k].wait_send()
        gathers[k].wait_send()
        send(back.at[pl.ds(BASE[k], CAP[k])], staged.at[pl.ds(HALF + BASE[k], CAP[k])], gs.at[k], gr.at[k], peers[k]).wait_recv()


def full_kernel(weights, staged, ss, rs):
    row, col = place()
    mate = at(across(row), col)
    greet([mate])
    copy = send(weights.at[pl.ds(HALF, HALF)], staged.at[pl.ds(0, HALF)], ss, rs, mate)
    copy.start()
    copy.wait()


STAGED = jax.ShapeDtypeStruct((HALF + SLOTS_S, G, G), F32)


def move(index, tables, weights):
    dma = pltpu.SemaphoreType.DMA
    if index == len(RUNGS):
        return pl.pallas_call(
            full_kernel,
            out_shape=STAGED,
            in_specs=[ANY],
            out_specs=ANY,
            scratch_shapes=[dma, dma],
            compiler_params=pltpu.CompilerParams(
                collective_id=2 + index, has_side_effects=True, vmem_limit_bytes=VMEM_LIMIT
            ),
            name="move_full",
        )(weights)
    size = RUNGS[index]
    m2 = size - M0 - M1

    def blocks(n):
        return pltpu.VMEM((n, G, G), F32)

    return pl.pallas_call(
        functools.partial(move_kernel, size),
        out_shape=STAGED,
        in_specs=[SMEM, ANY],
        out_specs=ANY,
        scratch_shapes=[
            blocks(HALF), blocks(SLOTS_S), blocks(SLOTS_S), blocks(M1), blocks(m2), blocks(M1), blocks(m2), blocks(SLOTS_S),
            dma((3,)), dma((9,)), dma((9,)), dma((3,)), dma((3,)), dma((9,)), dma((9,)),
        ],
        compiler_params=pltpu.CompilerParams(
            collective_id=2 + index, has_side_effects=True, vmem_limit_bytes=VMEM_LIMIT
        ),
        name=f"move_{size}",
    )(tables, weights)


CHUNK = 8
KP = 64


def split(value):
    high = value.astype(BF16)
    return high, (value - high.astype(F32)).astype(BF16)


def blocks_kernel(
    tables, pre, post, pidx, tab, rtab, ptab, weights, staged, new, cur, qs, ds, ps, scr, acc, win, wout, sem_in, sem_out
):
    steps = HALF // CHUNK

    def fetch(step, slot):
        for b in range(CHUNK):
            s = step * CHUNK + b
            moved = tables[6, s]

            @pl.when(moved == 0)
            def _():
                pltpu.make_async_copy(weights.at[s], win.at[slot, b], sem_in.at[slot]).start()

            @pl.when(moved == 1)
            def _():
                pltpu.make_async_copy(staged.at[tables[5, s]], win.at[slot, b], sem_in.at[slot]).start()

    fetch(0, 0)
    fetch(1, 1)
    neuron = lax.broadcasted_iota(I32, (1, G), 1)
    polarity = jnp.where(lax.rem(neuron, 5) == 4, -INHIB_GAIN, 1.0).astype(F32)

    use, supply, fast = tab[:, 10, :], tab[:, 11, :], tab[:, 12, :]
    scr[...] = jnp.zeros_like(scr)
    for t in range(STEPS):
        s = tab[:, t, :]
        use = BASE_USE + (use - BASE_USE) * USE_DECAY
        use = use + s * BASE_USE * (1.0 - use)
        release = s * use * supply
        supply = supply + SUPPLY_RATE * (1.0 - supply) - release
        fast = fast * PLUS_DECAY + s
        scr[:, t, :] = fast
        scr[:, STEPS + t, :] = release

    @pl.loop(0, ROWS)
    def _(g):
        terms = scr[g]
        high = terms.astype(BF16).astype(F32)
        low = terms - high
        qs[g] = jnp.concatenate([high[:20], low[:20], high[:20], jnp.zeros((4, G), F32)], axis=0).astype(BF16)
        driven = terms[STEPS : 2 * STEPS] * polarity
        dh = driven.astype(BF16).astype(F32)
        dl = driven - dh
        pad6 = jnp.zeros((6, G), F32)
        wide = jnp.concatenate([dh, pad6, dl, pad6, jnp.zeros((G - 32, G), F32)], axis=0)
        tall = jnp.transpose(wide)
        only = jnp.transpose(jnp.concatenate([dh, jnp.zeros((G - 10, G), F32)], axis=0))
        ds[g, pl.ds(0, G), :] = tall.astype(BF16)
        ds[g, pl.ds(G, G), :] = only.astype(BF16)

    for half, source in enumerate((rtab, ptab)):
        fast_p, slow_p = source[:, 13, :], source[:, 14, :]
        for t in range(STEPS):
            s = source[:, t, :]
            scr[pl.ds(half * COLS, COLS), t, :] = s * (PAIR_UP + TRIPLET_UP * slow_p)
            scr[pl.ds(half * COLS, COLS), STEPS + t, :] = -(PAIR_DOWN * fast_p)
            fast_p = fast_p * MINUS_DECAY + s
            slow_p = slow_p * SLOW_DECAY + s

    @pl.loop(0, 2 * COLS)
    def _(g):
        terms = scr[g] * LEARN_RATE
        high = terms.astype(BF16).astype(F32)
        low = terms - high
        rows = jnp.concatenate([high[:20], high[:20], low[:20], jnp.zeros((G - 60, G), F32)], axis=0)
        ps[g] = jnp.transpose(rows).astype(BF16)

    acc[...] = jnp.zeros_like(acc)

    @pl.loop(0, steps)
    def _(step):
        slot = lax.rem(step, 3)
        pltpu.make_async_copy(weights.at[pl.ds(0, CHUNK)], win.at[slot], sem_in.at[slot]).wait()

        @pl.when(step + 2 < steps)
        def _():
            fetch(step + 2, lax.rem(step + 2, 3))

        @pl.when(step >= 2)
        def _():
            pltpu.make_async_copy(wout.at[0], new.at[pl.ds(0, CHUNK)], sem_out.at[lax.rem(step, 2)]).wait()

        o = lax.rem(step, 2)
        currents = []
        for b in range(CHUNK):
            s = step * CHUNK + b
            moved, there = tables[6, s] == 1, tables[7, s]
            p = jnp.where(moved, pidx[0, there], pre[s])
            q = jnp.where(moved, pidx[1, there] + COLS, post[s])
            w = win[slot, b]
            change = jnp.dot(ps[q][:, :KP], qs[p], preferred_element_type=F32)
            wh, wl = split(w)
            currents.append((q, jnp.dot(jnp.concatenate([wh, wl], axis=1), ds[p], preferred_element_type=F32)))
            wout[o, b] = jnp.clip(w + change, 0.0, WEIGHT_MAX)
        for q, value in currents:
            acc[q] += value
        pltpu.make_async_copy(wout.at[o], new.at[pl.ds(step * CHUNK, CHUNK)], sem_out.at[o]).start()

    for q in range(2 * COLS):
        turned = jnp.transpose(acc[q])
        cur[q] = turned[0:16] + turned[16:32]
    for o in range(2):
        pltpu.make_async_copy(wout.at[o], new.at[pl.ds(0, CHUNK)], sem_out.at[o]).wait()


def do_blocks(tables, pre, post, pidx, tab, rtab, ptab, weights, staged):
    dma = pltpu.SemaphoreType.DMA
    return pl.pallas_call(
        blocks_kernel,
        out_shape=(jax.ShapeDtypeStruct((HALF, G, G), F32), jax.ShapeDtypeStruct((2 * COLS, 16, G), F32)),
        in_specs=[SMEM, SMEM, SMEM, SMEM, VMEM, VMEM, VMEM, ANY, ANY],
        out_specs=(ANY, VMEM),
        scratch_shapes=[
            pltpu.VMEM((ROWS, KP, G), BF16),
            pltpu.VMEM((ROWS, 2 * G, G), BF16),
            pltpu.VMEM((2 * COLS, G, G), BF16),
            pltpu.VMEM((ROWS, 24, G), F32),
            pltpu.VMEM((2 * COLS, G, G), F32),
            pltpu.VMEM((3, CHUNK, G, G), F32),
            pltpu.VMEM((2, CHUNK, G, G), F32),
            dma((3,)), dma((2,)),
        ],
        compiler_params=pltpu.CompilerParams(vmem_limit_bytes=VMEM_LIMIT),
        name="blocks",
    )(tables, pre, post, pidx, tab, rtab, ptab, weights, staged)


def currents_kernel(cur, out, got, ss, rs):
    row, col = place()
    far = across(row)
    peers, copies, arrivals = [], [], []
    for d in range(1, COLS):
        c = lax.rem(col + d, COLS)
        peers.append(at(row, c))
        copies.append(send(cur.at[c], got.at[col], ss.at[d], rs.at[col], at(row, c)))
        arrivals.append(send(cur.at[c], got.at[c], ss.at[d], rs.at[c], at(row, c)))
    for d in range(COLS):
        c = lax.rem(col + d, COLS)
        peers.append(at(far, c))
        copies.append(send(cur.at[COLS + c], got.at[COLS + col], ss.at[COLS + d], rs.at[COLS + col], at(far, c)))
        arrivals.append(send(cur.at[COLS + c], got.at[COLS + c], ss.at[COLS + d], rs.at[COLS + c], at(far, c)))
    greet(peers)
    for copy in copies:
        copy.start()
    got[col] = cur[col]
    for copy in arrivals:
        copy.wait()
    drive = got[0]
    for i in range(1, 2 * COLS):
        drive = drive + got[i]
    gain = 1.0 / math.sqrt(G * HALF)
    state = jnp.zeros((1, G), F32)
    for t in range(STEPS):
        state = state * SYN_DECAY + gain * drive[t : t + 1]
        out[pl.ds(t, 1), :] = state


def settle(cur):
    dma = pltpu.SemaphoreType.DMA
    return pl.pallas_call(
        currents_kernel,
        out_shape=jax.ShapeDtypeStruct((STEPS, G), F32),
        in_specs=[VMEM],
        out_specs=VMEM,
        scratch_shapes=[pltpu.VMEM((2 * COLS, 16, G), F32), dma((2 * COLS,)), dma((2 * COLS,))],
        compiler_params=pltpu.CompilerParams(collective_id=1, has_side_effects=True),
        name="currents",
    )(cur)


def body(spikes, stp_init, trace_init, weights, block_pre, block_post, block_count):
    own = weights[0, 0]
    pre, post = block_pre[0, 0], block_post[0, 0]
    held = block_count[0]
    pack = jnp.concatenate(
        [spikes.astype(F32), stp_init, trace_init, jnp.broadcast_to(held.astype(F32)[:, None], (1, G))], axis=0
    )
    idx = jnp.concatenate(
        [pre[None, HALF:], post[None, HALF:], jnp.zeros((6, G), I32)], axis=0
    )
    tab, rtab, ptab, pidx, cnt = exchange_tables(pack, idx)
    tables, rung = make_plan(cnt)
    staged = lax.switch(rung[0], [functools.partial(move, i) for i in range(len(RUNGS) + 1)], tables, own)
    new, cur = do_blocks(tables, pre, post, pidx, tab, rtab, ptab, own, staged)
    synaptic = settle(cur)
    return (new[None, None], synaptic)


def solution(mesh):
    placed = (
        P(None, ("row", "col")),
        P(None, ("row", "col")),
        P(None, ("row", "col")),
        P("row", "col", None, None, None),
        P("row", "col", None),
        P("row", "col", None),
        P("row", "col"),
    )
    return jax.shard_map(
        body,
        mesh=mesh,
        in_specs=placed,
        out_specs=(P("row", "col", None, None, None), P(None, ("row", "col"))),
        check_vma=False,
    )
```

```python
import functools
import math

import jax
import jax.numpy as jnp
from jax import lax
from jax.experimental import pallas as pl
from jax.experimental.pallas import tpu as pltpu
from jax.sharding import PartitionSpec as P

BASE_USE = 0.25
USE_DECAY = 0.98
SUPPLY_RATE = 0.005
PLUS_DECAY = math.exp(-1.0 / 16.8)
MINUS_DECAY = math.exp(-1.0 / 33.7)
SLOW_DECAY = math.exp(-1.0 / 114.0)
SYN_DECAY = math.exp(-1.0 / 5.0)
PAIR_UP = 1.0
TRIPLET_UP = 0.8
PAIR_DOWN = 0.9
LEARN_RATE = 0.02
WEIGHT_MAX = 1.0
INHIB_GAIN = 4.0

G = 128
HALF = 128
STEPS = 10
ROWS = 32
COLS = 4
MESH = pl.DeviceIdType.MESH
F32 = jnp.float32
I32 = jnp.int32
BF16 = jnp.bfloat16

EA = 4
EB = 4
ES = 32
FAR_A = 8 * EA
FAR_B = 8 * EB
SLOTS_B = FAR_B + ES
M0 = 12
RUNGS = ((16, 12, 37), (18, 14, 42), (26, 20, 60))
ITERS = 8
STEP_W = 10.0
INVERSE = (0, 3, 4, 1, 2, 7, 8, 5, 6)
ORDER = (1, 2, 3, 4, 5, 6, 7, 8, 0)
BASE_A = tuple([None] + [(k - 1) * EA for k in range(1, 9)])
BASE = tuple([FAR_B] + [(k - 1) * EB for k in range(1, 9)])
CAP = tuple([ES] + [EB] * 8)
VMEM_LIMIT = 60 * 1024 * 1024
ANY = pl.BlockSpec(memory_space=pl.ANY)
SMEM = pl.BlockSpec(memory_space=pltpu.SMEM)
VMEM = pl.BlockSpec(memory_space=pltpu.VMEM)


def place():
    row, col = lax.axis_index("row"), lax.axis_index("col")
    return row, col


def at(row, col):
    return {"row": row, "col": col}


def flip_core(row):
    return row + 1 - 2 * lax.rem(row, 2)


def across(row):
    return lax.rem(row + ROWS // 2, ROWS)


def shift_x(row, step):
    within = lax.rem(row, 8)
    return row - within + lax.rem(within + 2 * step + 8, 8)


def neighbour(k, row, col):
    if k == 0:
        return at(flip_core(row), col)
    which, other = (k - 1) // 2, (k - 1) % 2
    if which < 2:
        row = shift_x(row, 1 if which == 0 else -1)
    else:
        col = lax.rem(col + (1 if which == 2 else COLS - 1), COLS)
    return at(flip_core(row) if other else row, col)


def greet(peers):
    barrier = pltpu.get_barrier_semaphore()
    for peer in peers:
        pl.semaphore_signal(barrier, inc=1, device_id=peer, device_id_type=MESH)
    pl.semaphore_wait(barrier, len(peers))


def send(src, dst, send_sem, recv_sem, peer):
    return pltpu.make_async_remote_copy(
        src_ref=src, dst_ref=dst, send_sem=send_sem, recv_sem=recv_sem, device_id=peer, device_id_type=MESH
    )


def first_kernel(
    spikes, stp, trace, held, pre, post, weights,
    tab, rtab, ptab, pidx, tables, rung, z0, early,
    pack, idx, mine, cnt, s1, r1, s2, r2, s3, r3, s4, r4, s5, r5, s6, r6,
):
    row, col = place()
    far = across(row)
    mate = at(far, col)
    barrier = pltpu.get_barrier_semaphore()

    @pl.loop(1, ROWS)
    def _(d):
        peer = at(lax.rem(row + d, ROWS), col)
        pl.semaphore_signal(barrier, inc=1, device_id=peer, device_id_type=MESH)

    for d in range(1, COLS):
        c = lax.rem(col + d, COLS)
        pl.semaphore_signal(barrier, inc=1, device_id=at(row, c), device_id_type=MESH)
        pl.semaphore_signal(barrier, inc=1, device_id=at(far, c), device_id_type=MESH)
    for k in (6, 8):
        pl.semaphore_signal(barrier, inc=1, device_id=neighbour(k, row, col), device_id_type=MESH)

    count_row = jnp.broadcast_to(held[...].astype(F32), (1, G))
    pack[pl.ds(0, STEPS), :] = spikes[...].astype(F32)
    pack[pl.ds(10, 2), :] = stp[...]
    pack[pl.ds(12, 3), :] = trace[...]
    pack[pl.ds(15, 1), :] = count_row
    mine[...] = count_row
    idx[...] = jnp.concatenate([pre[pl.ds(1, 1), :], post[pl.ds(1, 1), :], jnp.zeros((6, G), I32)], axis=0)
    cnt[col, row] = count_row
    tab[row] = pack[...]
    rtab[col] = pack[...]
    pl.semaphore_wait(barrier, ROWS - 1 + 2 * (COLS - 1) + 2)

    @pl.loop(1, ROWS)
    def _(d):
        peer = at(lax.rem(row + d, ROWS), col)
        send(mine, cnt.at[col, row], s5.at[d], r5.at[row], peer).start()

    @pl.loop(1, ROWS)
    def _(d):
        peer = at(lax.rem(row + d, ROWS), col)
        send(pack, tab.at[row], s1.at[d], r1.at[row], peer).start()

    small = []
    for d in range(1, COLS):
        c = lax.rem(col + d, COLS)
        small.append(send(pack, rtab.at[col], s2.at[d], r2.at[col], at(row, c)))
    for d in range(COLS):
        c = lax.rem(col + d, COLS)
        small.append(send(pack, ptab.at[col], s3.at[d], r3.at[col], at(far, c)))
    last = send(idx, pidx, s4.at[0], r4.at[0], mate)
    small.append(last)
    for copy in small:
        copy.start()
    ahead = [send(weights.at[pl.ds(HALF, M0)], z0, s6.at[0], r6.at[0], mate)]
    for k in range(1, 9):
        ahead.append(
            send(
                weights.at[pl.ds(HALF + M0 + BASE_A[k], EA)],
                early.at[pl.ds(BASE_A[INVERSE[k]], EA)],
                s6.at[k], r6.at[INVERSE[k]], neighbour(k, row, col),
            )
        )
    for copy in ahead[:5]:
        copy.start()

    @pl.loop(1, ROWS)
    def _(d):
        source = lax.rem(row + d, ROWS)
        send(mine, cnt.at[col, source], s5.at[d], r5.at[source], at(source, col)).wait()

    for d in range(1, COLS):
        c = lax.rem(col + d, COLS)
        send(cnt.at[col], cnt.at[col], s4.at[d], r4.at[1 + col], at(row, c)).start()
    for copy in ahead[5:]:
        copy.start()
    for d in range(1, COLS):
        c = lax.rem(col + d, COLS)
        send(cnt.at[c], cnt.at[c], s4.at[d], r4.at[1 + c], at(row, c)).wait()

    make_plan(row, col, cnt, tables, rung)

    @pl.loop(1, ROWS)
    def _(d):
        source = lax.rem(row + d, ROWS)
        send(pack, tab.at[source], s1.at[d], r1.at[source], at(source, col)).wait()

    for d in range(1, COLS):
        c = lax.rem(col + d, COLS)
        send(pack, rtab.at[c], s2.at[d], r2.at[c], at(row, c)).wait()
    for d in range(COLS):
        c = lax.rem(col + d, COLS)
        send(pack, ptab.at[c], s3.at[d], r3.at[c], at(far, c)).wait()
    last.wait()
    ahead[0].wait()
    for k in range(1, 9):
        send(
            weights.at[pl.ds(HALF + M0 + BASE_A[k], EA)], early.at[pl.ds(BASE_A[k], EA)], s6.at[k], r6.at[k],
            neighbour(k, row, col),
        ).wait()


def first(spikes, stp, trace, held, pre, post, weights):
    dma = pltpu.SemaphoreType.DMA
    return pl.pallas_call(
        first_kernel,
        out_shape=(
            jax.ShapeDtypeStruct((ROWS, 16, G), F32),
            jax.ShapeDtypeStruct((COLS, 16, G), F32),
            jax.ShapeDtypeStruct((COLS, 16, G), F32),
            jax.ShapeDtypeStruct((8, G), I32),
            jax.ShapeDtypeStruct((8, G), I32),
            jax.ShapeDtypeStruct((1,), I32),
            jax.ShapeDtypeStruct((M0, G, G), F32),
            jax.ShapeDtypeStruct((FAR_A, G, G), F32),
        ),
        in_specs=[VMEM] * 6 + [ANY],
        out_specs=(VMEM, VMEM, VMEM, VMEM, VMEM, SMEM, ANY, ANY),
        scratch_shapes=[
            pltpu.VMEM((16, G), F32), pltpu.VMEM((8, G), I32), pltpu.VMEM((1, G), F32),
            pltpu.VMEM((COLS, ROWS, 1, G), F32),
            dma((ROWS,)), dma((ROWS,)), dma((COLS,)), dma((COLS,)), dma((COLS,)), dma((COLS,)),
            dma((COLS,)), dma((COLS + 1,)), dma((ROWS,)), dma((ROWS,)), dma((9,)), dma((9,)),
        ],
        compiler_params=pltpu.CompilerParams(
            collective_id=0, has_side_effects=True, vmem_limit_bytes=VMEM_LIMIT
        ),
        name="first",
    )(spikes, stp, trace, held, pre, post, weights)


def make_plan(row, col, cnt, tables, rung):
    shape = (8, G)
    lane = lax.broadcasted_iota(I32, shape, 1)
    slot = lax.broadcasted_iota(I32, (1, G), 1)

    def pick(r, total):
        for c in range(COLS):
            total = jnp.where(slot == c * ROWS + r, cnt[c, r], total)
        return total

    total = lax.fori_loop(0, ROWS, pick, jnp.zeros((1, G), F32))
    count = jnp.broadcast_to(total, shape)
    surplus = jnp.maximum(count - HALF, 0.0)
    core = lax.rem(lane, 2)
    x_at = lax.rem(lane, 8) // 2
    z_hi = lax.rem(lane, 32) // 16

    def roll(value, by):
        return pltpu.roll(value, by % G, 1)

    def from_sibling(v):
        return jnp.where(core == 0, roll(v, -1), roll(v, 1))

    def seen(v):
        same = (
            jnp.where(x_at == 3, roll(v, 6), roll(v, -2)),
            jnp.where(x_at == 0, roll(v, -6), roll(v, 2)),
            roll(v, -ROWS),
            roll(v, ROWS),
        )
        out = [from_sibling(v)]
        for value in same:
            out += [value, from_sibling(value)]
        return out

    def toward(which, v):
        if which == 0:
            return jnp.where(x_at == 3, roll(v, 6), roll(v, -2))
        if which == 1:
            return jnp.where(x_at == 0, roll(v, -6), roll(v, 2))
        return roll(v, -ROWS if which == 2 else ROWS)

    def arriving(v):
        out = [from_sibling(v[0])]
        for k in range(1, 9):
            value = toward((k - 1) // 2, v[INVERSE[k]])
            out.append(from_sibling(value) if (k - 1) % 2 else value)
        return out

    def add(values):
        return functools.reduce(jnp.add, values)

    zero = jnp.zeros(shape, F32)
    free = jnp.maximum(surplus - M0, 0.0)
    top_a = [zero] + [jnp.clip(surplus - float(M0 + BASE_A[k]), 0.0, float(EA)) for k in range(1, 9)]
    top = [top_a[k] + float(CAP[k]) for k in range(9)]
    outs, ins = [zero] * 9, [zero] * 9
    for _ in range(ITERS):
        load = jnp.maximum(surplus - add(outs), float(M0)) + add(ins)
        near = seen(load)
        outs = [jnp.clip(outs[k] + (load - near[k]) * (1.0 / STEP_W), 0.0, top[k]) for k in range(9)]
        scale = jnp.minimum(1.0, free / jnp.maximum(add(outs), 1e-6))
        outs = [v * scale for v in outs]
        ins = arriving(outs)
    give = [jnp.minimum(jnp.floor(v + 0.5), top[k]) for k, v in enumerate(outs)]
    over = jnp.maximum(add(give) - free, 0.0)
    for k in range(9):
        less = jnp.minimum(give[k], over)
        give[k] = give[k] - less
        over = over - less
    give_a = [jnp.minimum(give[k], top_a[k]) for k in range(9)]
    give_b = [give[k] - give_a[k] for k in range(9)]
    take_a, take_b = arriving(give_a), arriving(give_b)
    rest = free - add(give)
    in_a, in_b = add(take_a), add(take_b[1:])
    later = in_b + take_b[0]
    picked = jnp.int32(len(RUNGS))
    m1 = jnp.int32(RUNGS[-1][0])
    most_a, most_b = jnp.max(in_a), jnp.max(in_b)
    for i in reversed(range(len(RUNGS))):
        a, b, size = RUNGS[i]
        need = jnp.max(a + later + jnp.maximum(rest - (a - in_a), 0.0))
        fits = (most_a <= float(a)) & (most_b <= float(b)) & (need <= float(size))
        picked = jnp.where(fits, i, picked)
        m1 = jnp.where(fits, a, m1)
    full = picked == len(RUNGS)
    rung[0] = picked

    me = col * ROWS + row
    mate = col * ROWS + across(row)

    def of(v, who):
        return jnp.max(jnp.where(lane == who, v, -1.0), axis=1, keepdims=True).astype(I32)[:1]

    def table(i, value, most):
        tables[pl.ds(i, 1), :] = jnp.clip(value, 0, most)

    none = jnp.zeros((1, 1), I32)
    held = of(count, me)
    a_me = [none] + [of(give_a[k], me) for k in range(1, 9)]
    left_me = [none] + [of(top_a[k] - give_a[k], me) for k in range(1, 9)]
    rest_me = of(rest, me)
    left_total = add(left_me)

    def nth(r):
        j = M0 + FAR_A + r - left_total
        before = none
        for k in range(1, 9):
            here = (r >= before) & (r < before + left_me[k])
            j = jnp.where(here, M0 + BASE_A[k] + a_me[k] + r - before, j)
            before = before + left_me[k]
        return j

    chosen = jnp.zeros((1, G), I32)
    before = rest_me
    for k in ORDER:
        here = (slot >= BASE[k]) & (slot < BASE[k] + CAP[k])
        chosen = jnp.where(here, slot - BASE[k] + before, chosen)
        before = before + of(give_b[k], me)
    table(0, nth(chosen), HALF - 1)
    in_a_me, later_me = of(in_a, me), of(later, me)
    early_own = jnp.minimum(rest_me, m1 - in_a_me)
    table(1, nth(jnp.where(slot < m1, slot - in_a_me, early_own + slot - m1 - later_me)), HALF - 1)
    source = jnp.zeros((1, G), I32)
    kind = jnp.zeros((1, G), I32)
    before = none
    for k in range(1, 9):
        amount = of(take_a[k], me)
        here = (slot >= before) & (slot < before + amount)
        source = jnp.where(here, BASE_A[k] + slot - before, source)
        kind = jnp.where(here, 1, kind)
        before = before + amount
    before = none + m1
    for k in ORDER:
        amount = of(take_b[k], me)
        here = (slot >= before) & (slot < before + amount)
        source = jnp.where(here, BASE[k] + slot - before, source)
        kind = jnp.where(here, 1, kind)
        before = before + amount
    table(2, source, SLOTS_B - 1)
    table(3, kind, 1)
    gather = jnp.zeros((1, G), I32)
    before = none
    for k in range(1, 9):
        here = (slot >= BASE_A[k]) & (slot < BASE_A[k] + EA)
        gather = jnp.where(here, slot - BASE_A[k] + before, gather)
        before = before + of(take_a[k], mate)
    before = none
    for k in ORDER:
        here = (slot >= FAR_A + BASE[k]) & (slot < FAR_A + BASE[k] + CAP[k])
        gather = jnp.where(here, slot - FAR_A - BASE[k] + before, gather)
        before = before + of(take_b[k], mate)
    table(4, gather, HALF - 1)
    j = slot - held
    in_a_mate, later_mate, rest_mate = of(in_a, mate), of(later, mate), of(rest, mate)
    early_mate = jnp.minimum(rest_mate, m1 - in_a_mate)
    total_left = none
    r = jnp.zeros((1, G), I32)
    by_a = jnp.zeros((1, G), I32)
    for k in range(1, 9):
        a_mate, left = of(give_a[k], mate), of(top_a[k] - give_a[k], mate)
        i = j - (M0 + BASE_A[k])
        here = (i >= 0) & (i < EA)
        by_a = jnp.where(here & (i < a_mate), 1, by_a)
        r = jnp.where(here, total_left + i - a_mate, r)
        total_left = total_left + left
    r = jnp.where(j >= M0 + FAR_A, total_left + j - (M0 + FAR_A), r)
    spot = jnp.where(r < early_mate, in_a_mate + r, m1 + later_mate + r - early_mate)
    before = rest_mate
    for k in ORDER:
        amount = of(give_b[k], mate)
        here = (r >= before) & (r < before + amount)
        spot = jnp.where(here, HALF + FAR_A + BASE[k] + r - before, spot)
        before = before + amount
    spot = jnp.where(by_a == 1, HALF + j - M0, spot)
    spot = jnp.where(full, j, spot)
    kind = jnp.where(j < 0, 0, jnp.where((j < M0) & jnp.logical_not(full), 2, 1))
    spot = jnp.where(kind == 2, j, spot)
    table(5, spot, HALF + FAR_A + SLOTS_B - 1)
    table(6, kind, 2)
    table(7, j, HALF - 1)


def move_kernel(
    sizes, tables, weights, early, staged,
    up, held_a, spread, imports, z1, z2, z3, got1, got2, got3, back, ls, ss, rs, zs, zr, gs, gr, as_, ar,
):
    m1, m2, size = sizes
    m3 = size - m1 - m2
    row, col = place()
    mate = at(across(row), col)
    peers = [neighbour(k, row, col) for k in range(9)]
    load = pltpu.make_async_copy(weights.at[pl.ds(HALF, HALF)], up, ls.at[0])
    load.start()
    load_a = pltpu.make_async_copy(early, held_a, ls.at[1])
    load_a.start()
    greet(peers + [mate])
    load_a.wait()
    load.wait()
    first_z = send(z1, got1, zs.at[0], zr.at[0], mate)
    second_z = send(z2, got2, zs.at[1], zr.at[1], mate)
    third_z = send(z3, got3, zs.at[2], zr.at[2], mate)

    @pl.loop(0, m1)
    def _(i):
        z1[i] = jnp.where(tables[3, i] == 1, held_a[jnp.minimum(tables[2, i], FAR_A - 1)], up[tables[1, i]])

    first_z.start()
    spreads = [
        send(spread.at[pl.ds(BASE[k], CAP[k])], imports.at[pl.ds(BASE[INVERSE[k]], CAP[k])], ss.at[k], rs.at[INVERSE[k]], peers[k])
        for k in range(9)
    ]
    for k in ORDER:

        @pl.loop(BASE[k], BASE[k] + CAP[k])
        def _(i):
            spread[i] = up[tables[0, i]]

        spreads[k].start()
    for k in range(9):
        send(spread.at[pl.ds(BASE[k], CAP[k])], imports.at[pl.ds(BASE[k], CAP[k])], ss.at[k], rs.at[k], peers[k]).wait_recv()

    def fill(target, start, count):
        @pl.loop(0, count)
        def _(i):
            t = start + i
            target[i] = jnp.where(tables[3, t] == 1, imports[tables[2, t]], up[tables[1, t]])

    fill(z2, m1, m2)
    second_z.start()
    fill(z3, m1 + m2, m3)
    third_z.start()

    def onward(k, part):
        if part == 0:
            base, there, n, s, r = BASE_A[k], BASE_A[INVERSE[k]], EA, as_, ar
        else:
            base, there, n, s, r = FAR_A + BASE[k], FAR_A + BASE[INVERSE[k]], CAP[k], gs, gr
        go = send(back.at[pl.ds(base, n)], staged.at[pl.ds(HALF + there, n)], s.at[k], r.at[INVERSE[k]], peers[k])
        come = send(back.at[pl.ds(base, n)], staged.at[pl.ds(HALF + base, n)], s.at[k], r.at[k], peers[k])
        return base, n, go, come

    waits = []
    first_z.wait_recv()
    for k in range(1, 9):
        base, n, go, come = onward(k, 0)

        @pl.loop(base, base + n)
        def _(i):
            back[i] = got1[jnp.minimum(tables[4, i], m1 - 1)]

        go.start()
        waits.append(come)
    out1 = pltpu.make_async_copy(got1, staged.at[pl.ds(0, m1)], ls.at[1])
    out1.start()
    second_z.wait_recv()
    for k in range(1, 9):
        base, n, go, come = onward(k, 1)

        @pl.loop(base, base + n)
        def _(i):
            back[i] = got2[jnp.minimum(tables[4, i], m2 - 1)]

        go.start()
        waits.append(come)
    out2 = pltpu.make_async_copy(got2, staged.at[pl.ds(m1, m2)], ls.at[2])
    out2.start()
    third_z.wait_recv()
    out3 = pltpu.make_async_copy(got3, staged.at[pl.ds(m1 + m2, m3)], ls.at[3])
    out3.start()
    base, n, go, come = onward(0, 1)

    @pl.loop(base, base + n)
    def _(i):
        t = tables[4, i]
        back[i] = jnp.where(t < m2, got2[jnp.minimum(t, m2 - 1)], got3[jnp.clip(t - m2, 0, m3 - 1)])

    go.start()
    waits.append(come)
    out1.wait()
    out2.wait()
    out3.wait()
    first_z.wait_send()
    second_z.wait_send()
    third_z.wait_send()
    for k in range(9):
        spreads[k].wait_send()
    for come in waits:
        come.wait()


def full_kernel(weights, staged, ss, rs):
    row, col = place()
    mate = at(across(row), col)
    greet([mate])
    copy = send(weights.at[pl.ds(HALF, HALF)], staged.at[pl.ds(0, HALF)], ss, rs, mate)
    copy.start()
    copy.wait()


STAGED = jax.ShapeDtypeStruct((HALF + FAR_A + SLOTS_B, G, G), F32)


def move(index, tables, weights, early):
    dma = pltpu.SemaphoreType.DMA
    if index == len(RUNGS):
        return pl.pallas_call(
            full_kernel,
            out_shape=STAGED,
            in_specs=[ANY],
            out_specs=ANY,
            scratch_shapes=[dma, dma],
            compiler_params=pltpu.CompilerParams(
                collective_id=2 + index, has_side_effects=True, vmem_limit_bytes=VMEM_LIMIT
            ),
            name="move_full",
        )(weights)
    m1, m2, size = RUNGS[index]
    m3 = size - m1 - m2

    def blocks(n):
        return pltpu.VMEM((n, G, G), F32)

    return pl.pallas_call(
        functools.partial(move_kernel, RUNGS[index]),
        out_shape=STAGED,
        in_specs=[SMEM, ANY, ANY],
        out_specs=ANY,
        scratch_shapes=[
            blocks(HALF), blocks(FAR_A), blocks(SLOTS_B), blocks(SLOTS_B), blocks(m1), blocks(m2), blocks(m3),
            blocks(m1), blocks(m2), blocks(m3), blocks(FAR_A + SLOTS_B),
            dma((4,)), dma((9,)), dma((9,)), dma((3,)), dma((3,)), dma((9,)), dma((9,)), dma((9,)), dma((9,)),
        ],
        compiler_params=pltpu.CompilerParams(
            collective_id=2 + index, has_side_effects=True, vmem_limit_bytes=VMEM_LIMIT
        ),
        name=f"move_{size}",
    )(tables, weights, early)


CHUNK = 8
KP = 64


def split(value):
    high = value.astype(BF16)
    return high, (value - high.astype(F32)).astype(BF16)


def blocks_kernel(
    tables, pre, post, pidx, tab, rtab, ptab, weights, staged, z0, new, cur, qs, ds, ps, scr, acc, win, wout, sem_in, sem_out
):
    steps = HALF // CHUNK

    def fetch(step, slot):
        for b in range(CHUNK):
            s = step * CHUNK + b
            moved = tables[6, s]

            @pl.when(moved == 0)
            def _():
                pltpu.make_async_copy(weights.at[s], win.at[slot, b], sem_in.at[slot]).start()

            @pl.when(moved == 1)
            def _():
                pltpu.make_async_copy(staged.at[tables[5, s]], win.at[slot, b], sem_in.at[slot]).start()

            @pl.when(moved == 2)
            def _():
                pltpu.make_async_copy(z0.at[jnp.minimum(tables[5, s], M0 - 1)], win.at[slot, b], sem_in.at[slot]).start()

    fetch(0, 0)
    fetch(1, 1)
    neuron = lax.broadcasted_iota(I32, (1, G), 1)
    lane = lax.broadcasted_iota(I32, (G, G), 1)
    polarity = jnp.where(lax.rem(neuron, 5) == 4, -INHIB_GAIN, 1.0).astype(F32)

    use, supply, fast = tab[:, 10, :], tab[:, 11, :], tab[:, 12, :]
    scr[...] = jnp.zeros_like(scr)
    for t in range(STEPS):
        s = tab[:, t, :]
        use = BASE_USE + (use - BASE_USE) * USE_DECAY
        use = use + s * BASE_USE * (1.0 - use)
        release = s * use * supply
        supply = supply + SUPPLY_RATE * (1.0 - supply) - release
        fast = fast * PLUS_DECAY + s
        scr[:, t, :] = fast
        scr[:, STEPS + t, :] = release

    @pl.loop(0, ROWS, unroll=8)
    def _(g):
        terms = scr[g]
        high = terms.astype(BF16).astype(F32)
        low = terms - high
        qs[g] = jnp.concatenate([high[:20], low[:20], high[:20], jnp.zeros((4, G), F32)], axis=0).astype(BF16)
        driven = terms[STEPS : 2 * STEPS] * polarity
        dh = driven.astype(BF16).astype(F32)
        dl = driven - dh
        pad6 = jnp.zeros((6, G), F32)
        wide = jnp.concatenate([dh, pad6, dl, pad6, jnp.zeros((G - 32, G), F32)], axis=0)
        tall = jnp.transpose(wide)
        only = jnp.where(lane < 16, tall, 0.0)
        ds[g, pl.ds(0, G), :] = tall.astype(BF16)
        ds[g, pl.ds(G, G), :] = only.astype(BF16)

    for half, source in enumerate((rtab, ptab)):
        fast_p, slow_p = source[:, 13, :], source[:, 14, :]
        for t in range(STEPS):
            s = source[:, t, :]
            scr[pl.ds(half * COLS, COLS), t, :] = s * (PAIR_UP + TRIPLET_UP * slow_p)
            scr[pl.ds(half * COLS, COLS), STEPS + t, :] = -(PAIR_DOWN * fast_p)
            fast_p = fast_p * MINUS_DECAY + s
            slow_p = slow_p * SLOW_DECAY + s

    @pl.loop(0, 2 * COLS, unroll=8)
    def _(g):
        terms = scr[g] * LEARN_RATE
        high = terms.astype(BF16).astype(F32)
        low = terms - high
        rows = jnp.concatenate([high[:20], high[:20], low[:20], jnp.zeros((G - 60, G), F32)], axis=0)
        ps[g] = jnp.transpose(rows).astype(BF16)

    acc[...] = jnp.zeros_like(acc)

    @pl.loop(0, steps)
    def _(step):
        slot = lax.rem(step, 3)
        pltpu.make_async_copy(weights.at[pl.ds(0, CHUNK)], win.at[slot], sem_in.at[slot]).wait()

        @pl.when(step + 2 < steps)
        def _():
            fetch(step + 2, lax.rem(step + 2, 3))

        @pl.when(step >= 2)
        def _():
            pltpu.make_async_copy(wout.at[0], new.at[pl.ds(0, CHUNK)], sem_out.at[lax.rem(step, 2)]).wait()

        o = lax.rem(step, 2)
        currents = []
        for b in range(CHUNK):
            s = step * CHUNK + b
            moved, there = tables[6, s] >= 1, tables[7, s]
            p = jnp.where(moved, pidx[0, there], pre[s])
            q = jnp.where(moved, pidx[1, there] + COLS, post[s])
            w = win[slot, b]
            change = jnp.dot(ps[q][:, :KP], qs[p], preferred_element_type=F32)
            wh, wl = split(w)
            currents.append((q, jnp.dot(jnp.concatenate([wh, wl], axis=1), ds[p], preferred_element_type=F32)))
            wout[o, b] = jnp.clip(w + change, 0.0, WEIGHT_MAX)
        for q, value in currents:
            acc[q] += value
        pltpu.make_async_copy(wout.at[o], new.at[pl.ds(step * CHUNK, CHUNK)], sem_out.at[o]).start()

    for q in range(2 * COLS):
        turned = jnp.transpose(acc[q])
        cur[q] = turned[0:16] + turned[16:32]
    for o in range(2):
        pltpu.make_async_copy(wout.at[o], new.at[pl.ds(0, CHUNK)], sem_out.at[o]).wait()


def do_blocks(tables, pre, post, pidx, tab, rtab, ptab, weights, staged, z0):
    dma = pltpu.SemaphoreType.DMA
    return pl.pallas_call(
        blocks_kernel,
        out_shape=(jax.ShapeDtypeStruct((HALF, G, G), F32), jax.ShapeDtypeStruct((2 * COLS, 16, G), F32)),
        in_specs=[SMEM, SMEM, SMEM, SMEM, VMEM, VMEM, VMEM, ANY, ANY, ANY],
        out_specs=(ANY, VMEM),
        scratch_shapes=[
            pltpu.VMEM((ROWS, KP, G), BF16),
            pltpu.VMEM((ROWS, 2 * G, G), BF16),
            pltpu.VMEM((2 * COLS, G, G), BF16),
            pltpu.VMEM((ROWS, 24, G), F32),
            pltpu.VMEM((2 * COLS, G, G), F32),
            pltpu.VMEM((3, CHUNK, G, G), F32),
            pltpu.VMEM((2, CHUNK, G, G), F32),
            dma((3,)), dma((2,)),
        ],
        compiler_params=pltpu.CompilerParams(vmem_limit_bytes=VMEM_LIMIT),
        name="blocks",
    )(tables, pre, post, pidx, tab, rtab, ptab, weights, staged, z0)


def currents_kernel(cur, out, got, ss, rs):
    row, col = place()
    far = across(row)
    peers, copies, arrivals = [], [], []
    for d in range(1, COLS):
        c = lax.rem(col + d, COLS)
        peers.append(at(row, c))
        copies.append(send(cur.at[c], got.at[col], ss.at[d], rs.at[col], at(row, c)))
        arrivals.append(send(cur.at[c], got.at[c], ss.at[d], rs.at[c], at(row, c)))
    for d in range(COLS):
        c = lax.rem(col + d, COLS)
        peers.append(at(far, c))
        copies.append(send(cur.at[COLS + c], got.at[COLS + col], ss.at[COLS + d], rs.at[COLS + col], at(far, c)))
        arrivals.append(send(cur.at[COLS + c], got.at[COLS + c], ss.at[COLS + d], rs.at[COLS + c], at(far, c)))
    greet(peers)
    for copy in copies:
        copy.start()
    got[col] = cur[col]
    for copy in arrivals:
        copy.wait()
    drive = got[0]
    for i in range(1, 2 * COLS):
        drive = drive + got[i]
    gain = 1.0 / math.sqrt(G * HALF)
    state = jnp.zeros((1, G), F32)
    for t in range(STEPS):
        state = state * SYN_DECAY + gain * drive[t : t + 1]
        out[pl.ds(t, 1), :] = state


def settle(cur):
    dma = pltpu.SemaphoreType.DMA
    return pl.pallas_call(
        currents_kernel,
        out_shape=jax.ShapeDtypeStruct((STEPS, G), F32),
        in_specs=[VMEM],
        out_specs=VMEM,
        scratch_shapes=[pltpu.VMEM((2 * COLS, 16, G), F32), dma((2 * COLS,)), dma((2 * COLS,))],
        compiler_params=pltpu.CompilerParams(collective_id=1, has_side_effects=True),
        name="currents",
    )(cur)


def body(spikes, stp_init, trace_init, weights, block_pre, block_post, block_count):
    own = weights[0, 0]
    pre, post = block_pre[0, 0], block_post[0, 0]
    tab, rtab, ptab, pidx, tables, rung, z0, early = first(
        spikes, stp_init, trace_init, block_count, pre.reshape(2, G), post.reshape(2, G), own
    )
    staged = lax.switch(
        rung[0], [functools.partial(move, i) for i in range(len(RUNGS) + 1)], tables, own, early
    )
    new, cur = do_blocks(tables, pre, post, pidx, tab, rtab, ptab, own, staged, z0)
    synaptic = settle(cur)
    return (new[None, None], synaptic)


def solution(mesh):
    placed = (
        P(None, ("row", "col")),
        P(None, ("row", "col")),
        P(None, ("row", "col")),
        P("row", "col", None, None, None),
        P("row", "col", None),
        P("row", "col", None),
        P("row", "col"),
    )
    return jax.shard_map(
        body,
        mesh=mesh,
        in_specs=placed,
        out_specs=(P("row", "col", None, None, None), P(None, ("row", "col"))),
        check_vma=False,
    )
```

```python
import functools
import math

import jax
import jax.numpy as jnp
from jax import lax
from jax.experimental import pallas as pl
from jax.experimental.pallas import tpu as pltpu
from jax.sharding import PartitionSpec as P

BASE_USE = 0.25
USE_DECAY = 0.98
SUPPLY_RATE = 0.005
PLUS_DECAY = math.exp(-1.0 / 16.8)
MINUS_DECAY = math.exp(-1.0 / 33.7)
SLOW_DECAY = math.exp(-1.0 / 114.0)
SYN_DECAY = math.exp(-1.0 / 5.0)
PAIR_UP = 1.0
TRIPLET_UP = 0.8
PAIR_DOWN = 0.9
LEARN_RATE = 0.02
WEIGHT_MAX = 1.0
INHIB_GAIN = 4.0

G = 128
HALF = 128
STEPS = 10
ROWS = 32
COLS = 4
MESH = pl.DeviceIdType.MESH
F32 = jnp.float32
I32 = jnp.int32
BF16 = jnp.bfloat16

EA = 4
EB = 3
ES = 28
M0 = 16
RUNGS = ((16, 22, 29, 31), (16, 24, 32, 36), (20, 32, 42, 46))
M0_FIRST = 6
ITERS = 8
STEP_W = 8.0
INVERSE = (0, 3, 4, 1, 2, 7, 8, 5, 6)
RANGES = tuple(
    [(k, EA, (k - 1) * EA) for k in range(1, 9)]
    + [(k, EB, 8 * EA + (k - 1) * EB) for k in range(1, 9)]
    + [(0, ES, 8 * (EA + EB))]
)
BACK = tuple([INVERSE[k] - 1 for k in range(1, 9)] + [7 + INVERSE[k] for k in range(1, 9)] + [16])
SPREAD = 8 * (EA + EB) + ES
VMEM_LIMIT = 60 * 1024 * 1024
ANY = pl.BlockSpec(memory_space=pl.ANY)
SMEM = pl.BlockSpec(memory_space=pltpu.SMEM)
VMEM = pl.BlockSpec(memory_space=pltpu.VMEM)


def place():
    row, col = lax.axis_index("row"), lax.axis_index("col")
    return row, col


def at(row, col):
    return {"row": row, "col": col}


def flip_core(row):
    return row + 1 - 2 * lax.rem(row, 2)


def across(row):
    return lax.rem(row + ROWS // 2, ROWS)


def shift_x(row, step):
    within = lax.rem(row, 8)
    return row - within + lax.rem(within + 2 * step + 8, 8)


def neighbour(k, row, col):
    if k == 0:
        return at(flip_core(row), col)
    which, other = (k - 1) // 2, (k - 1) % 2
    if which < 2:
        row = shift_x(row, 1 if which == 0 else -1)
    else:
        col = lax.rem(col + (1 if which == 2 else COLS - 1), COLS)
    return at(flip_core(row) if other else row, col)


def greet(peers):
    barrier = pltpu.get_barrier_semaphore()
    for peer in peers:
        pl.semaphore_signal(barrier, inc=1, device_id=peer, device_id_type=MESH)
    pl.semaphore_wait(barrier, len(peers))


def send(src, dst, send_sem, recv_sem, peer):
    return pltpu.make_async_remote_copy(
        src_ref=src, dst_ref=dst, send_sem=send_sem, recv_sem=recv_sem, device_id=peer, device_id_type=MESH
    )


def first_kernel(
    spikes, stp, trace, held, pre, post, weights,
    tab, rtab, ptab, pidx, tables, rung, z0, early,
    pack, idx, cnt, s1, r1, s2, r2, s3, r3, s4, r4, s5, r5, s6, r6, s7, r7, s8, r8,
):
    row, col = place()
    far = across(row)
    mate = at(far, col)
    barrier = pltpu.get_barrier_semaphore()

    plane, within = row // 8, lax.rem(row, 8)

    def in_plane(d):
        return plane * 8 + lax.rem(within + d, 8)

    for d in range(1, 8):
        pl.semaphore_signal(barrier, inc=1, device_id=at(in_plane(d), col), device_id_type=MESH)
    for d in range(1, 4):
        pl.semaphore_signal(barrier, inc=1, device_id=at(lax.rem(row + 8 * d, ROWS), col), device_id_type=MESH)
    for d in range(1, COLS):
        c = lax.rem(col + d, COLS)
        pl.semaphore_signal(barrier, inc=1, device_id=at(row, c), device_id_type=MESH)
        pl.semaphore_signal(barrier, inc=1, device_id=at(far, c), device_id_type=MESH)
    for k in (6, 8):
        pl.semaphore_signal(barrier, inc=1, device_id=neighbour(k, row, col), device_id_type=MESH)

    count_row = jnp.broadcast_to(held[...].astype(F32), (1, G))
    pack[pl.ds(0, STEPS), :] = spikes[...].astype(F32)
    pack[pl.ds(10, 2), :] = stp[...]
    pack[pl.ds(12, 3), :] = trace[...]
    pack[pl.ds(15, 1), :] = count_row
    idx[...] = jnp.concatenate([pre[pl.ds(1, 1), :], post[pl.ds(1, 1), :], jnp.zeros((6, G), I32)], axis=0)
    cnt[row, col] = count_row
    tab[row] = pack[...]
    rtab[col] = pack[...]
    pl.semaphore_wait(barrier, 7 + 3 + 2 * (COLS - 1) + 2)

    for d in range(1, COLS):
        c = lax.rem(col + d, COLS)
        send(cnt.at[row, col], cnt.at[row, col], s4.at[d], r4.at[1 + col], at(row, c)).start()
    z_parts = [
        send(weights.at[pl.ds(HALF + a, n)], z0.at[pl.ds(a, n)], s6.at[17 + i], r6.at[17 + i], mate)
        for i, (a, n) in enumerate(((0, M0_FIRST), (M0_FIRST, M0 - M0_FIRST)))
    ]
    z_parts[0].start()
    ahead = []
    for i, (k, n, base) in enumerate(RANGES):
        there = RANGES[BACK[i]][2]
        ahead.append(
            send(
                weights.at[pl.ds(HALF + M0 + base, n)], early.at[pl.ds(there, n)],
                s6.at[i], r6.at[BACK[i]], neighbour(k, row, col),
            )
        )
    along_y = [copy for copy, (k, _, _) in zip(ahead, RANGES) if k > 4]
    others = [copy for copy, (k, _, _) in zip(ahead, RANGES) if k <= 4]
    for d in range(1, COLS):
        c = lax.rem(col + d, COLS)
        send(pack, rtab.at[col], s2.at[d], r2.at[col], at(row, c)).start()
    for copy in along_y:
        copy.start()
    for d in range(1, COLS):
        c = lax.rem(col + d, COLS)
        send(cnt.at[row, c], cnt.at[row, c], s4.at[d], r4.at[1 + c], at(row, c)).wait()

    for d in range(1, 8):
        send(cnt.at[row], cnt.at[row], s5.at[d], r5.at[within], at(in_plane(d), col)).start()
    for d in range(1, 8):
        send(pack, tab.at[row], s1.at[d], r1.at[within], at(in_plane(d), col)).start()
    for copy in others:
        copy.start()
    for d in range(1, 8):
        source = in_plane(d)
        send(cnt.at[source], cnt.at[source], s5.at[d], r5.at[lax.rem(within + d, 8)], at(source, col)).wait()
    ours = pl.ds(plane * 8, 8)
    for d in range(1, 4):
        peer = at(lax.rem(row + 8 * d, ROWS), col)
        send(cnt.at[ours], cnt.at[ours], s7.at[d], r7.at[plane], peer).start()
    for d in range(COLS):
        c = lax.rem(col + d, COLS)
        send(pack, ptab.at[col], s3.at[d], r3.at[col], at(far, c)).start()
    last = send(idx, pidx, s4.at[0], r4.at[0], mate)
    last.start()
    for d in range(1, 8):
        source = in_plane(d)
        send(pack, tab.at[source], s1.at[d], r1.at[lax.rem(within + d, 8)], at(source, col)).wait()
    for d in range(1, 4):
        peer = at(lax.rem(row + 8 * d, ROWS), col)
        send(tab.at[ours], tab.at[ours], s8.at[d], r8.at[plane], peer).start()
    z_parts[1].start()
    for d in range(1, 4):
        p = lax.rem(plane + d, 4)
        theirs = pl.ds(p * 8, 8)
        send(cnt.at[theirs], cnt.at[theirs], s7.at[d], r7.at[p], at(lax.rem(row + 8 * d, ROWS), col)).wait()

    make_plan(row, col, cnt, tables, rung)

    for d in range(1, 4):
        p = lax.rem(plane + d, 4)
        theirs = pl.ds(p * 8, 8)
        send(tab.at[theirs], tab.at[theirs], s8.at[d], r8.at[p], at(lax.rem(row + 8 * d, ROWS), col)).wait()
    for d in range(1, COLS):
        c = lax.rem(col + d, COLS)
        send(pack, rtab.at[c], s2.at[d], r2.at[c], at(row, c)).wait()
    for d in range(COLS):
        c = lax.rem(col + d, COLS)
        send(pack, ptab.at[c], s3.at[d], r3.at[c], at(far, c)).wait()
    last.wait()
    for part in z_parts:
        part.wait()
    for i, (k, n, base) in enumerate(RANGES):
        send(
            weights.at[pl.ds(HALF + M0 + base, n)], early.at[pl.ds(base, n)], s6.at[i], r6.at[i], neighbour(k, row, col)
        ).wait()


def first(spikes, stp, trace, held, pre, post, weights):
    dma = pltpu.SemaphoreType.DMA
    return pl.pallas_call(
        first_kernel,
        out_shape=(
            jax.ShapeDtypeStruct((ROWS, 16, G), F32),
            jax.ShapeDtypeStruct((COLS, 16, G), F32),
            jax.ShapeDtypeStruct((COLS, 16, G), F32),
            jax.ShapeDtypeStruct((8, G), I32),
            jax.ShapeDtypeStruct((8, G), I32),
            jax.ShapeDtypeStruct((1,), I32),
            jax.ShapeDtypeStruct((M0, G, G), F32),
            jax.ShapeDtypeStruct((SPREAD, G, G), F32),
        ),
        in_specs=[VMEM] * 6 + [ANY],
        out_specs=(VMEM, VMEM, VMEM, VMEM, VMEM, SMEM, ANY, ANY),
        scratch_shapes=[
            pltpu.VMEM((16, G), F32), pltpu.VMEM((8, G), I32),
            pltpu.VMEM((ROWS, COLS, 1, G), F32),
            dma((8,)), dma((8,)), dma((COLS,)), dma((COLS,)), dma((COLS,)), dma((COLS,)),
            dma((COLS,)), dma((COLS + 1,)), dma((8,)), dma((8,)), dma((19,)), dma((19,)),
            dma((4,)), dma((4,)), dma((4,)), dma((4,)),
        ],
        compiler_params=pltpu.CompilerParams(
            collective_id=0, has_side_effects=True, vmem_limit_bytes=VMEM_LIMIT
        ),
        name="first",
    )(spikes, stp, trace, held, pre, post, weights)


def make_plan(row, col, cnt, tables, rung):
    shape = (8, G)
    lane = lax.broadcasted_iota(I32, shape, 1)
    slot = lax.broadcasted_iota(I32, (1, G), 1)

    def pick(r, total):
        for c in range(COLS):
            total = jnp.where(slot == c * ROWS + r, cnt[r, c], total)
        return total

    total = lax.fori_loop(0, ROWS, pick, jnp.zeros((1, G), F32))
    count = jnp.broadcast_to(total, shape)
    surplus = jnp.maximum(count - HALF, 0.0)
    core = lax.rem(lane, 2)
    x_at = lax.rem(lane, 8) // 2
    z_hi = lax.rem(lane, 32) // 16

    def roll(value, by):
        return pltpu.roll(value, by % G, 1)

    def from_sibling(v):
        return jnp.where(core == 0, roll(v, -1), roll(v, 1))

    def seen(v):
        same = (
            jnp.where(x_at == 3, roll(v, 6), roll(v, -2)),
            jnp.where(x_at == 0, roll(v, -6), roll(v, 2)),
            roll(v, -ROWS),
            roll(v, ROWS),
        )
        out = [from_sibling(v)]
        for value in same:
            out += [value, from_sibling(value)]
        return out

    def toward(which, v):
        if which == 0:
            return jnp.where(x_at == 3, roll(v, 6), roll(v, -2))
        if which == 1:
            return jnp.where(x_at == 0, roll(v, -6), roll(v, 2))
        return roll(v, -ROWS if which == 2 else ROWS)

    def arriving(v):
        out = [from_sibling(v[0])]
        for k in range(1, 9):
            value = toward((k - 1) // 2, v[INVERSE[k]])
            out.append(from_sibling(value) if (k - 1) % 2 else value)
        return out

    def add(values):
        return functools.reduce(jnp.add, values)

    zero = jnp.zeros(shape, F32)
    free = jnp.maximum(surplus - M0, 0.0)
    tops = [jnp.clip(surplus - float(M0 + base), 0.0, float(n)) for _, n, base in RANGES]
    top_a = [zero] + tops[:8]
    top = [tops[16]] + [tops[i] + tops[8 + i] for i in range(8)]
    outs, ins = [zero] * 9, [zero] * 9
    for _ in range(ITERS):
        load = jnp.maximum(surplus - add(outs), float(M0)) + add(ins)
        near = seen(load)
        outs = [jnp.clip(outs[k] + (load - near[k]) * (1.0 / STEP_W), 0.0, top[k]) for k in range(9)]
        scale = jnp.minimum(1.0, free / jnp.maximum(add(outs), 1e-6))
        outs = [v * scale for v in outs]
        ins = arriving(outs)
    give = [jnp.minimum(jnp.floor(v + 0.5), top[k]) for k, v in enumerate(outs)]
    over = jnp.maximum(add(give) - free, 0.0)
    for k in range(9):
        less = jnp.minimum(give[k], over)
        give[k] = give[k] - less
        over = over - less
    give_a = [jnp.minimum(give[k], top_a[k]) for k in range(9)]
    give_b = [give[k] - give_a[k] for k in range(9)]
    take_a, take_b = arriving(give_a), arriving(give_b)
    gives = give_a[1:] + give_b[1:] + give_b[:1]
    takes = take_a[1:] + take_b[1:] + take_b[:1]
    lefts = [tops[i] - gives[i] for i in range(17)]
    in_a = add(takes[:8])
    in_ab = in_a + add(takes[8:16])
    in_all = in_ab + takes[16]
    most = [jnp.max(v) for v in (in_a, in_ab, in_all, in_all + free - add(give))]
    picked = jnp.int32(len(RUNGS))
    for i in reversed(range(len(RUNGS))):
        fits = functools.reduce(jnp.logical_and, [m <= float(n) for m, n in zip(most, RUNGS[i])])
        picked = jnp.where(fits, i, picked)
    full = picked == len(RUNGS)
    rung[0] = picked

    me = col * ROWS + row
    mate = col * ROWS + across(row)

    def of(v, who):
        return jnp.max(jnp.where(lane == who, v, -1.0), axis=1, keepdims=True).astype(I32)[:1]

    def table(i, value, most):
        tables[pl.ds(i, 1), :] = jnp.clip(value, 0, most)

    none = jnp.zeros((1, 1), I32)
    held = of(count, me)
    give_me = [of(v, me) for v in gives]
    left_me = [of(v, me) for v in lefts]
    in_me = of(in_all, me)
    r = slot - in_me
    j = M0 + SPREAD + r - add(left_me)
    before = none
    for i, (_, _, base) in enumerate(RANGES):
        here = (r >= before) & (r < before + left_me[i])
        j = jnp.where(here, M0 + base + give_me[i] + r - before, j)
        before = before + left_me[i]
    table(1, j, HALF - 1)
    source = jnp.zeros((1, G), I32)
    kind = jnp.zeros((1, G), I32)
    gather = jnp.zeros((1, G), I32)
    before, ahead = none, none
    for i, (_, n, base) in enumerate(RANGES):
        amount = of(takes[i], me)
        here = (slot >= before) & (slot < before + amount)
        source = jnp.where(here, base + slot - before, source)
        kind = jnp.where(here, 1, kind)
        before = before + amount
        here = (slot >= base) & (slot < base + n)
        gather = jnp.where(here, slot - base + ahead, gather)
        ahead = ahead + of(takes[i], mate)
    table(2, source, SPREAD - 1)
    table(3, kind, 1)
    table(4, gather, HALF - 1)
    table(0, slot, HALF - 1)
    j = slot - held
    left = none
    r = jnp.zeros((1, G), I32)
    passed = jnp.zeros((1, G), I32)
    for i, (_, n, base) in enumerate(RANGES):
        amount = of(gives[i], mate)
        inside = j - (M0 + base)
        here = (inside >= 0) & (inside < n)
        passed = jnp.where(here & (inside < amount), 1, passed)
        r = jnp.where(here, left + inside - amount, r)
        left = left + of(lefts[i], mate)
    r = jnp.where(j >= M0 + SPREAD, left + j - (M0 + SPREAD), r)
    spot = jnp.where(passed == 1, HALF + j - M0, of(in_all, mate) + r)
    spot = jnp.where(full, j, spot)
    kind = jnp.where(j < 0, 0, jnp.where((j < M0) & jnp.logical_not(full), 2, 1))
    spot = jnp.where(kind == 2, j, spot)
    table(5, spot, HALF + SPREAD - 1)
    table(6, kind, 2)
    table(7, j, HALF - 1)


def move_kernel(ends, tables, weights, early, staged, up, held, back, *rest):
    outs, gots = rest[:4], rest[4:8]
    ls, zs, zr, gs, gr = rest[8:]
    starts = (0,) + ends[:3]
    row, col = place()
    mate = at(across(row), col)
    peers = [neighbour(k, row, col) for k in range(9)]
    load = pltpu.make_async_copy(weights.at[pl.ds(HALF, HALF)], up, ls.at[0])
    load.start()
    load_early = pltpu.make_async_copy(early, held, ls.at[1])
    load_early.start()
    greet(peers + [mate])
    load_early.wait()
    load.wait()
    zs_all = [send(outs[i], gots[i], zs.at[i], zr.at[i], mate) for i in range(4)]
    for part in range(4):
        start, target = starts[part], outs[part]

        @pl.loop(0, ends[part] - start)
        def _(i):
            t = start + i
            target[i] = jnp.where(tables[3, t] == 1, held[tables[2, t]], up[tables[1, t]])

        zs_all[part].start()

    def received(t, parts):
        value = gots[0][jnp.minimum(t, ends[0] - 1)]
        for p in range(1, parts):
            size = ends[p] - starts[p]
            value = jnp.where(t < starts[p], value, gots[p][jnp.clip(t - starts[p], 0, size - 1)])
        return value

    waits, stores = [], []
    for part in range(4):
        zs_all[part].wait_recv()
        for i, (k, n, base) in enumerate(RANGES):
            if i // 8 != part:
                continue

            @pl.loop(base, base + n)
            def _(slot):
                back[slot] = received(tables[4, slot], part + 1)

            there = RANGES[BACK[i]][2]
            send(
                back.at[pl.ds(base, n)], staged.at[pl.ds(HALF + there, n)], gs.at[i], gr.at[BACK[i]], peers[k]
            ).start()
            waits.append(send(back.at[pl.ds(base, n)], staged.at[pl.ds(HALF + base, n)], gs.at[i], gr.at[i], peers[k]))
        store = pltpu.make_async_copy(
            gots[part], staged.at[pl.ds(starts[part], ends[part] - starts[part])], ls.at[2 + part]
        )
        store.start()
        stores.append(store)
    for store in stores:
        store.wait()
    for copy in zs_all:
        copy.wait_send()
    for come in waits:
        come.wait()


def full_kernel(weights, staged, ss, rs):
    row, col = place()
    mate = at(across(row), col)
    greet([mate])
    copy = send(weights.at[pl.ds(HALF, HALF)], staged.at[pl.ds(0, HALF)], ss, rs, mate)
    copy.start()
    copy.wait()


STAGED = jax.ShapeDtypeStruct((HALF + SPREAD, G, G), F32)


def move(index, tables, weights, early):
    dma = pltpu.SemaphoreType.DMA
    if index == len(RUNGS):
        return pl.pallas_call(
            full_kernel,
            out_shape=STAGED,
            in_specs=[ANY],
            out_specs=ANY,
            scratch_shapes=[dma, dma],
            compiler_params=pltpu.CompilerParams(
                collective_id=2 + index, has_side_effects=True, vmem_limit_bytes=VMEM_LIMIT
            ),
            name="move_full",
        )(weights)
    ends = RUNGS[index]

    def blocks(n):
        return pltpu.VMEM((n, G, G), F32)

    parts = [blocks(b - a) for a, b in zip((0,) + ends[:3], ends)]
    return pl.pallas_call(
        functools.partial(move_kernel, ends),
        out_shape=STAGED,
        in_specs=[SMEM, ANY, ANY],
        out_specs=ANY,
        scratch_shapes=[
            blocks(HALF), blocks(SPREAD), blocks(SPREAD), *parts, *parts,
            dma((6,)), dma((4,)), dma((4,)), dma((17,)), dma((17,)),
        ],
        compiler_params=pltpu.CompilerParams(
            collective_id=2 + index, has_side_effects=True, vmem_limit_bytes=VMEM_LIMIT
        ),
        name=f"move_{ends[3]}",
    )(tables, weights, early)


CHUNK = 8
KP = 64


def split(value):
    high = value.astype(BF16)
    return high, (value - high.astype(F32)).astype(BF16)


def blocks_kernel(
    tables, pre, post, pidx, tab, rtab, ptab, weights, staged, z0, new, cur, qs, ds, ps, scr, acc, win, wout, sem_in, sem_out
):
    steps = HALF // CHUNK

    def fetch(step, slot):
        for b in range(CHUNK):
            s = step * CHUNK + b
            moved = tables[6, s]

            @pl.when(moved == 0)
            def _():
                pltpu.make_async_copy(weights.at[s], win.at[slot, b], sem_in.at[slot]).start()

            @pl.when(moved == 1)
            def _():
                pltpu.make_async_copy(staged.at[tables[5, s]], win.at[slot, b], sem_in.at[slot]).start()

            @pl.when(moved == 2)
            def _():
                pltpu.make_async_copy(z0.at[jnp.minimum(tables[5, s], M0 - 1)], win.at[slot, b], sem_in.at[slot]).start()

    fetch(0, 0)
    fetch(1, 1)
    neuron = lax.broadcasted_iota(I32, (1, G), 1)
    lane = lax.broadcasted_iota(I32, (G, G), 1)
    polarity = jnp.where(lax.rem(neuron, 5) == 4, -INHIB_GAIN, 1.0).astype(F32)

    use, supply, fast = tab[:, 10, :], tab[:, 11, :], tab[:, 12, :]
    scr[...] = jnp.zeros_like(scr)
    for t in range(STEPS):
        s = tab[:, t, :]
        use = BASE_USE + (use - BASE_USE) * USE_DECAY
        use = use + s * BASE_USE * (1.0 - use)
        release = s * use * supply
        supply = supply + SUPPLY_RATE * (1.0 - supply) - release
        fast = fast * PLUS_DECAY + s
        scr[:, t, :] = fast
        scr[:, STEPS + t, :] = release

    @pl.loop(0, ROWS, unroll=8)
    def _(g):
        terms = scr[g]
        high = terms.astype(BF16).astype(F32)
        low = terms - high
        qs[g] = jnp.concatenate([high[:20], low[:20], high[:20], jnp.zeros((4, G), F32)], axis=0).astype(BF16)
        driven = terms[STEPS : 2 * STEPS] * polarity
        dh = driven.astype(BF16).astype(F32)
        dl = driven - dh
        pad6 = jnp.zeros((6, G), F32)
        wide = jnp.concatenate([dh, pad6, dl, pad6, jnp.zeros((G - 32, G), F32)], axis=0)
        tall = jnp.transpose(wide)
        only = jnp.where(lane < 16, tall, 0.0)
        ds[g, pl.ds(0, G), :] = tall.astype(BF16)
        ds[g, pl.ds(G, G), :] = only.astype(BF16)

    for half, source in enumerate((rtab, ptab)):
        fast_p, slow_p = source[:, 13, :], source[:, 14, :]
        for t in range(STEPS):
            s = source[:, t, :]
            scr[pl.ds(half * COLS, COLS), t, :] = s * (PAIR_UP + TRIPLET_UP * slow_p)
            scr[pl.ds(half * COLS, COLS), STEPS + t, :] = -(PAIR_DOWN * fast_p)
            fast_p = fast_p * MINUS_DECAY + s
            slow_p = slow_p * SLOW_DECAY + s

    @pl.loop(0, 2 * COLS, unroll=8)
    def _(g):
        terms = scr[g] * LEARN_RATE
        high = terms.astype(BF16).astype(F32)
        low = terms - high
        rows = jnp.concatenate([high[:20], high[:20], low[:20], jnp.zeros((G - 60, G), F32)], axis=0)
        ps[g] = jnp.transpose(rows).astype(BF16)

    acc[...] = jnp.zeros_like(acc)

    @pl.loop(0, steps)
    def _(step):
        slot = lax.rem(step, 3)
        pltpu.make_async_copy(weights.at[pl.ds(0, CHUNK)], win.at[slot], sem_in.at[slot]).wait()

        @pl.when(step + 2 < steps)
        def _():
            fetch(step + 2, lax.rem(step + 2, 3))

        @pl.when(step >= 2)
        def _():
            pltpu.make_async_copy(wout.at[0], new.at[pl.ds(0, CHUNK)], sem_out.at[lax.rem(step, 2)]).wait()

        o = lax.rem(step, 2)
        currents = []
        for b in range(CHUNK):
            s = step * CHUNK + b
            moved, there = tables[6, s] >= 1, tables[7, s]
            p = jnp.where(moved, pidx[0, there], pre[s])
            q = jnp.where(moved, pidx[1, there] + COLS, post[s])
            w = win[slot, b]
            change = jnp.dot(ps[q][:, :KP], qs[p], preferred_element_type=F32)
            wh, wl = split(w)
            currents.append((q, jnp.dot(jnp.concatenate([wh, wl], axis=1), ds[p], preferred_element_type=F32)))
            wout[o, b] = jnp.clip(w + change, 0.0, WEIGHT_MAX)
        for q, value in currents:
            acc[q] += value
        pltpu.make_async_copy(wout.at[o], new.at[pl.ds(step * CHUNK, CHUNK)], sem_out.at[o]).start()

    for q in range(2 * COLS):
        turned = jnp.transpose(acc[q])
        cur[q] = turned[0:16] + turned[16:32]
    for o in range(2):
        pltpu.make_async_copy(wout.at[o], new.at[pl.ds(0, CHUNK)], sem_out.at[o]).wait()


def do_blocks(tables, pre, post, pidx, tab, rtab, ptab, weights, staged, z0):
    dma = pltpu.SemaphoreType.DMA
    return pl.pallas_call(
        blocks_kernel,
        out_shape=(jax.ShapeDtypeStruct((HALF, G, G), F32), jax.ShapeDtypeStruct((2 * COLS, 16, G), F32)),
        in_specs=[SMEM, SMEM, SMEM, SMEM, VMEM, VMEM, VMEM, ANY, ANY, ANY],
        out_specs=(ANY, VMEM),
        scratch_shapes=[
            pltpu.VMEM((ROWS, KP, G), BF16),
            pltpu.VMEM((ROWS, 2 * G, G), BF16),
            pltpu.VMEM((2 * COLS, G, G), BF16),
            pltpu.VMEM((ROWS, 24, G), F32),
            pltpu.VMEM((2 * COLS, G, G), F32),
            pltpu.VMEM((3, CHUNK, G, G), F32),
            pltpu.VMEM((2, CHUNK, G, G), F32),
            dma((3,)), dma((2,)),
        ],
        compiler_params=pltpu.CompilerParams(vmem_limit_bytes=VMEM_LIMIT),
        name="blocks",
    )(tables, pre, post, pidx, tab, rtab, ptab, weights, staged, z0)


def currents_kernel(cur, out, got, ss, rs):
    row, col = place()
    far = across(row)
    peers, copies, arrivals = [], [], []
    for d in range(1, COLS):
        c = lax.rem(col + d, COLS)
        peers.append(at(row, c))
        copies.append(send(cur.at[c], got.at[col], ss.at[d], rs.at[col], at(row, c)))
        arrivals.append(send(cur.at[c], got.at[c], ss.at[d], rs.at[c], at(row, c)))
    for d in range(COLS):
        c = lax.rem(col + d, COLS)
        peers.append(at(far, c))
        copies.append(send(cur.at[COLS + c], got.at[COLS + col], ss.at[COLS + d], rs.at[COLS + col], at(far, c)))
        arrivals.append(send(cur.at[COLS + c], got.at[COLS + c], ss.at[COLS + d], rs.at[COLS + c], at(far, c)))
    greet(peers)
    for copy in copies:
        copy.start()
    got[col] = cur[col]
    for copy in arrivals:
        copy.wait()
    drive = got[0]
    for i in range(1, 2 * COLS):
        drive = drive + got[i]
    gain = 1.0 / math.sqrt(G * HALF)
    state = jnp.zeros((1, G), F32)
    for t in range(STEPS):
        state = state * SYN_DECAY + gain * drive[t : t + 1]
        out[pl.ds(t, 1), :] = state


def settle(cur):
    dma = pltpu.SemaphoreType.DMA
    return pl.pallas_call(
        currents_kernel,
        out_shape=jax.ShapeDtypeStruct((STEPS, G), F32),
        in_specs=[VMEM],
        out_specs=VMEM,
        scratch_shapes=[pltpu.VMEM((2 * COLS, 16, G), F32), dma((2 * COLS,)), dma((2 * COLS,))],
        compiler_params=pltpu.CompilerParams(collective_id=1, has_side_effects=True),
        name="currents",
    )(cur)


def body(spikes, stp_init, trace_init, weights, block_pre, block_post, block_count):
    own = weights[0, 0]
    pre, post = block_pre[0, 0], block_post[0, 0]
    tab, rtab, ptab, pidx, tables, rung, z0, early = first(
        spikes, stp_init, trace_init, block_count, pre.reshape(2, G), post.reshape(2, G), own
    )
    staged = lax.switch(
        rung[0], [functools.partial(move, i) for i in range(len(RUNGS) + 1)], tables, own, early
    )
    new, cur = do_blocks(tables, pre, post, pidx, tab, rtab, ptab, own, staged, z0)
    synaptic = settle(cur)
    return (new[None, None], synaptic)


def solution(mesh):
    placed = (
        P(None, ("row", "col")),
        P(None, ("row", "col")),
        P(None, ("row", "col")),
        P("row", "col", None, None, None),
        P("row", "col", None),
        P("row", "col", None),
        P("row", "col"),
    )
    return jax.shard_map(
        body,
        mesh=mesh,
        in_specs=placed,
        out_specs=(P("row", "col", None, None, None), P(None, ("row", "col"))),
        check_vma=False,
    )
```

```python
import functools
import math

import jax
import jax.numpy as jnp
from jax import lax
from jax.experimental import pallas as pl
from jax.experimental.pallas import tpu as pltpu
from jax.sharding import PartitionSpec as P

BASE_USE = 0.25
USE_DECAY = 0.98
SUPPLY_RATE = 0.005
PLUS_DECAY = math.exp(-1.0 / 16.8)
MINUS_DECAY = math.exp(-1.0 / 33.7)
SLOW_DECAY = math.exp(-1.0 / 114.0)
SYN_DECAY = math.exp(-1.0 / 5.0)
PAIR_UP = 1.0
TRIPLET_UP = 0.8
PAIR_DOWN = 0.9
LEARN_RATE = 0.02
WEIGHT_MAX = 1.0
INHIB_GAIN = 4.0

G = 128
HALF = 128
STEPS = 10
ROWS = 32
COLS = 4
MESH = pl.DeviceIdType.MESH
F32 = jnp.float32
I32 = jnp.int32
BF16 = jnp.bfloat16

EA = 4
EB = 3
ES = 32
M0 = 16
RUNGS = ((16, 22, 28, 30), (16, 23, 29, 32), (17, 25, 31, 35), (20, 32, 40, 44))
M0_FIRST = 6
ITERS = 12
STEP_W = 10.0
INVERSE = (0, 3, 4, 1, 2, 7, 8, 5, 6)
RANGES = tuple(
    [(k, EA, (k - 1) * EA) for k in range(1, 9)]
    + [(k, EB, 8 * EA + (k - 1) * EB) for k in range(1, 9)]
    + [(0, ES, 8 * (EA + EB))]
)
BACK = tuple([INVERSE[k] - 1 for k in range(1, 9)] + [7 + INVERSE[k] for k in range(1, 9)] + [16])
SPREAD = 8 * (EA + EB) + ES
VMEM_LIMIT = 60 * 1024 * 1024
ANY = pl.BlockSpec(memory_space=pl.ANY)
SMEM = pl.BlockSpec(memory_space=pltpu.SMEM)
VMEM = pl.BlockSpec(memory_space=pltpu.VMEM)


def place():
    row, col = lax.axis_index("row"), lax.axis_index("col")
    return row, col


def at(row, col):
    return {"row": row, "col": col}


def flip_core(row):
    return row + 1 - 2 * lax.rem(row, 2)


def across(row):
    return lax.rem(row + ROWS // 2, ROWS)


def shift_x(row, step):
    within = lax.rem(row, 8)
    return row - within + lax.rem(within + 2 * step + 8, 8)


def neighbour(k, row, col):
    if k == 0:
        return at(flip_core(row), col)
    which, other = (k - 1) // 2, (k - 1) % 2
    if which < 2:
        row = shift_x(row, 1 if which == 0 else -1)
    else:
        col = lax.rem(col + (1 if which == 2 else COLS - 1), COLS)
    return at(flip_core(row) if other else row, col)


def greet(peers):
    barrier = pltpu.get_barrier_semaphore()
    for peer in peers:
        pl.semaphore_signal(barrier, inc=1, device_id=peer, device_id_type=MESH)
    pl.semaphore_wait(barrier, len(peers))


def send(src, dst, send_sem, recv_sem, peer):
    return pltpu.make_async_remote_copy(
        src_ref=src, dst_ref=dst, send_sem=send_sem, recv_sem=recv_sem, device_id=peer, device_id_type=MESH
    )


def first_kernel(
    spikes, stp, trace, held, pre, post, weights,
    tab, rtab, ptab, pidx, tables, rung, z0, early,
    pack, idx, cnt, s1, r1, s2, r2, s3, r3, s4, r4, s5, r5, s6, r6, s7, r7, s8, r8,
):
    row, col = place()
    far = across(row)
    mate = at(far, col)
    barrier = pltpu.get_barrier_semaphore()

    plane, within = row // 8, lax.rem(row, 8)

    def in_plane(d):
        return plane * 8 + lax.rem(within + d, 8)

    for d in range(1, 8):
        pl.semaphore_signal(barrier, inc=1, device_id=at(in_plane(d), col), device_id_type=MESH)
    for d in range(1, 4):
        pl.semaphore_signal(barrier, inc=1, device_id=at(lax.rem(row + 8 * d, ROWS), col), device_id_type=MESH)
    for d in range(1, COLS):
        c = lax.rem(col + d, COLS)
        pl.semaphore_signal(barrier, inc=1, device_id=at(row, c), device_id_type=MESH)
        pl.semaphore_signal(barrier, inc=1, device_id=at(far, c), device_id_type=MESH)
    for k in (6, 8):
        pl.semaphore_signal(barrier, inc=1, device_id=neighbour(k, row, col), device_id_type=MESH)

    count_row = jnp.broadcast_to(held[...].astype(F32), (1, G))
    pack[pl.ds(0, STEPS), :] = spikes[...].astype(F32)
    pack[pl.ds(10, 2), :] = stp[...]
    pack[pl.ds(12, 3), :] = trace[...]
    pack[pl.ds(15, 1), :] = count_row
    idx[...] = jnp.concatenate([pre[pl.ds(1, 1), :], post[pl.ds(1, 1), :], jnp.zeros((6, G), I32)], axis=0)
    cnt[row, col] = count_row
    tab[row] = pack[...]
    rtab[col] = pack[...]
    pl.semaphore_wait(barrier, 7 + 3 + 2 * (COLS - 1) + 2)

    for d in range(1, COLS):
        c = lax.rem(col + d, COLS)
        send(cnt.at[row, col], cnt.at[row, col], s4.at[d], r4.at[1 + col], at(row, c)).start()
    z_parts = [
        send(weights.at[pl.ds(HALF + a, n)], z0.at[pl.ds(a, n)], s6.at[17 + i], r6.at[17 + i], mate)
        for i, (a, n) in enumerate(((0, M0_FIRST), (M0_FIRST, M0 - M0_FIRST)))
    ]
    z_parts[0].start()
    ahead = []
    for i, (k, n, base) in enumerate(RANGES):
        there = RANGES[BACK[i]][2]
        ahead.append(
            send(
                weights.at[pl.ds(HALF + M0 + base, n)], early.at[pl.ds(there, n)],
                s6.at[i], r6.at[BACK[i]], neighbour(k, row, col),
            )
        )
    along_y = [copy for copy, (k, _, _) in zip(ahead, RANGES) if k > 4]
    others = [copy for copy, (k, _, _) in zip(ahead, RANGES) if k <= 4]
    for d in range(1, COLS):
        c = lax.rem(col + d, COLS)
        send(pack, rtab.at[col], s2.at[d], r2.at[col], at(row, c)).start()
    for copy in along_y:
        copy.start()
    for d in range(1, COLS):
        c = lax.rem(col + d, COLS)
        send(cnt.at[row, c], cnt.at[row, c], s4.at[d], r4.at[1 + c], at(row, c)).wait()

    for d in range(1, 8):
        send(cnt.at[row], cnt.at[row], s5.at[d], r5.at[within], at(in_plane(d), col)).start()
    for d in range(1, 8):
        send(pack, tab.at[row], s1.at[d], r1.at[within], at(in_plane(d), col)).start()
    for copy in others:
        copy.start()
    for d in range(1, 8):
        source = in_plane(d)
        send(cnt.at[source], cnt.at[source], s5.at[d], r5.at[lax.rem(within + d, 8)], at(source, col)).wait()
    ours = pl.ds(plane * 8, 8)
    for d in range(1, 4):
        peer = at(lax.rem(row + 8 * d, ROWS), col)
        send(cnt.at[ours], cnt.at[ours], s7.at[d], r7.at[plane], peer).start()
    for d in range(COLS):
        c = lax.rem(col + d, COLS)
        send(pack, ptab.at[col], s3.at[d], r3.at[col], at(far, c)).start()
    last = send(idx, pidx, s4.at[0], r4.at[0], mate)
    last.start()
    for d in range(1, 8):
        source = in_plane(d)
        send(pack, tab.at[source], s1.at[d], r1.at[lax.rem(within + d, 8)], at(source, col)).wait()
    for d in range(1, 4):
        peer = at(lax.rem(row + 8 * d, ROWS), col)
        send(tab.at[ours], tab.at[ours], s8.at[d], r8.at[plane], peer).start()
    z_parts[1].start()
    for d in range(1, 4):
        p = lax.rem(plane + d, 4)
        theirs = pl.ds(p * 8, 8)
        send(cnt.at[theirs], cnt.at[theirs], s7.at[d], r7.at[p], at(lax.rem(row + 8 * d, ROWS), col)).wait()

    make_plan(row, col, cnt, tables, rung)

    for d in range(1, 4):
        p = lax.rem(plane + d, 4)
        theirs = pl.ds(p * 8, 8)
        send(tab.at[theirs], tab.at[theirs], s8.at[d], r8.at[p], at(lax.rem(row + 8 * d, ROWS), col)).wait()
    for d in range(1, COLS):
        c = lax.rem(col + d, COLS)
        send(pack, rtab.at[c], s2.at[d], r2.at[c], at(row, c)).wait()
    for d in range(COLS):
        c = lax.rem(col + d, COLS)
        send(pack, ptab.at[c], s3.at[d], r3.at[c], at(far, c)).wait()
    last.wait()
    for part in z_parts:
        part.wait()
    for i, (k, n, base) in enumerate(RANGES):
        send(
            weights.at[pl.ds(HALF + M0 + base, n)], early.at[pl.ds(base, n)], s6.at[i], r6.at[i], neighbour(k, row, col)
        ).wait()


def first(spikes, stp, trace, held, pre, post, weights):
    dma = pltpu.SemaphoreType.DMA
    return pl.pallas_call(
        first_kernel,
        out_shape=(
            jax.ShapeDtypeStruct((ROWS, 16, G), F32),
            jax.ShapeDtypeStruct((COLS, 16, G), F32),
            jax.ShapeDtypeStruct((COLS, 16, G), F32),
            jax.ShapeDtypeStruct((8, G), I32),
            jax.ShapeDtypeStruct((8, G), I32),
            jax.ShapeDtypeStruct((1,), I32),
            jax.ShapeDtypeStruct((M0, G, G), F32),
            jax.ShapeDtypeStruct((SPREAD, G, G), F32),
        ),
        in_specs=[VMEM] * 6 + [ANY],
        out_specs=(VMEM, VMEM, VMEM, VMEM, VMEM, SMEM, ANY, ANY),
        scratch_shapes=[
            pltpu.VMEM((16, G), F32), pltpu.VMEM((8, G), I32),
            pltpu.VMEM((ROWS, COLS, 1, G), F32),
            dma((8,)), dma((8,)), dma((COLS,)), dma((COLS,)), dma((COLS,)), dma((COLS,)),
            dma((COLS,)), dma((COLS + 1,)), dma((8,)), dma((8,)), dma((19,)), dma((19,)),
            dma((4,)), dma((4,)), dma((4,)), dma((4,)),
        ],
        compiler_params=pltpu.CompilerParams(
            collective_id=0, has_side_effects=True, vmem_limit_bytes=VMEM_LIMIT
        ),
        name="first",
    )(spikes, stp, trace, held, pre, post, weights)


def make_plan(row, col, cnt, tables, rung):
    shape = (8, G)
    lane = lax.broadcasted_iota(I32, shape, 1)
    slot = lax.broadcasted_iota(I32, (1, G), 1)

    def pick(r, total):
        for c in range(COLS):
            total = jnp.where(slot == c * ROWS + r, cnt[r, c], total)
        return total

    total = lax.fori_loop(0, ROWS, pick, jnp.zeros((1, G), F32))
    count = jnp.broadcast_to(total, shape)
    surplus = jnp.maximum(count - HALF, 0.0)
    core = lax.rem(lane, 2)
    x_at = lax.rem(lane, 8) // 2
    z_hi = lax.rem(lane, 32) // 16

    def roll(value, by):
        return pltpu.roll(value, by % G, 1)

    def from_sibling(v):
        return jnp.where(core == 0, roll(v, -1), roll(v, 1))

    def seen(v):
        same = (
            jnp.where(x_at == 3, roll(v, 6), roll(v, -2)),
            jnp.where(x_at == 0, roll(v, -6), roll(v, 2)),
            roll(v, -ROWS),
            roll(v, ROWS),
        )
        out = [from_sibling(v)]
        for value in same:
            out += [value, from_sibling(value)]
        return out

    def toward(which, v):
        if which == 0:
            return jnp.where(x_at == 3, roll(v, 6), roll(v, -2))
        if which == 1:
            return jnp.where(x_at == 0, roll(v, -6), roll(v, 2))
        return roll(v, -ROWS if which == 2 else ROWS)

    def arriving(v):
        out = [from_sibling(v[0])]
        for k in range(1, 9):
            value = toward((k - 1) // 2, v[INVERSE[k]])
            out.append(from_sibling(value) if (k - 1) % 2 else value)
        return out

    def add(values):
        return functools.reduce(jnp.add, values)

    zero = jnp.zeros(shape, F32)
    free = jnp.maximum(surplus - M0, 0.0)
    tops = [jnp.clip(surplus - float(M0 + base), 0.0, float(n)) for _, n, base in RANGES]
    top_a = [zero] + tops[:8]
    top = [tops[16]] + [tops[i] + tops[8 + i] for i in range(8)]
    outs, ins = [zero] * 9, [zero] * 9
    for _ in range(ITERS):
        load = jnp.maximum(surplus - add(outs), float(M0)) + add(ins)
        near = seen(load)
        outs = [jnp.clip(outs[k] + (load - near[k]) * (1.0 / STEP_W), 0.0, top[k]) for k in range(9)]
        scale = jnp.minimum(1.0, free / jnp.maximum(add(outs), 1e-6))
        outs = [v * scale for v in outs]
        ins = arriving(outs)
    give = [jnp.minimum(jnp.floor(v + 0.5), top[k]) for k, v in enumerate(outs)]
    over = jnp.maximum(add(give) - free, 0.0)
    for k in range(9):
        less = jnp.minimum(give[k], over)
        give[k] = give[k] - less
        over = over - less
    give_a = [jnp.minimum(give[k], top_a[k]) for k in range(9)]
    give_b = [give[k] - give_a[k] for k in range(9)]
    take_a, take_b = arriving(give_a), arriving(give_b)
    gives = give_a[1:] + give_b[1:] + give_b[:1]
    takes = take_a[1:] + take_b[1:] + take_b[:1]
    lefts = [tops[i] - gives[i] for i in range(17)]
    in_a = add(takes[:8])
    in_ab = in_a + add(takes[8:16])
    in_all = in_ab + takes[16]
    most = [jnp.max(v) for v in (in_a, in_ab, in_all, in_all + free - add(give))]
    picked = jnp.int32(len(RUNGS))
    for i in reversed(range(len(RUNGS))):
        fits = functools.reduce(jnp.logical_and, [m <= float(n) for m, n in zip(most, RUNGS[i])])
        picked = jnp.where(fits, i, picked)
    full = picked == len(RUNGS)
    rung[0] = picked

    me = col * ROWS + row
    mate = col * ROWS + across(row)

    def of(v, who):
        return jnp.max(jnp.where(lane == who, v, -1.0), axis=1, keepdims=True).astype(I32)[:1]

    def table(i, value, most):
        tables[pl.ds(i, 1), :] = jnp.clip(value, 0, most)

    none = jnp.zeros((1, 1), I32)
    held = of(count, me)
    give_me = [of(v, me) for v in gives]
    left_me = [of(v, me) for v in lefts]
    in_me = of(in_all, me)
    r = slot - in_me
    j = M0 + SPREAD + r - add(left_me)
    before = none
    for i, (_, _, base) in enumerate(RANGES):
        here = (r >= before) & (r < before + left_me[i])
        j = jnp.where(here, M0 + base + give_me[i] + r - before, j)
        before = before + left_me[i]
    table(1, j, HALF - 1)
    source = jnp.zeros((1, G), I32)
    kind = jnp.zeros((1, G), I32)
    gather = jnp.zeros((1, G), I32)
    before, ahead = none, none
    for i, (_, n, base) in enumerate(RANGES):
        amount = of(takes[i], me)
        here = (slot >= before) & (slot < before + amount)
        source = jnp.where(here, base + slot - before, source)
        kind = jnp.where(here, 1, kind)
        before = before + amount
        here = (slot >= base) & (slot < base + n)
        gather = jnp.where(here, slot - base + ahead, gather)
        ahead = ahead + of(takes[i], mate)
    table(2, source, SPREAD - 1)
    table(3, kind, 1)
    table(4, gather, HALF - 1)
    table(0, slot, HALF - 1)
    j = slot - held
    left = none
    r = jnp.zeros((1, G), I32)
    passed = jnp.zeros((1, G), I32)
    for i, (_, n, base) in enumerate(RANGES):
        amount = of(gives[i], mate)
        inside = j - (M0 + base)
        here = (inside >= 0) & (inside < n)
        passed = jnp.where(here & (inside < amount), 1, passed)
        r = jnp.where(here, left + inside - amount, r)
        left = left + of(lefts[i], mate)
    r = jnp.where(j >= M0 + SPREAD, left + j - (M0 + SPREAD), r)
    spot = jnp.where(passed == 1, HALF + j - M0, of(in_all, mate) + r)
    spot = jnp.where(full, j, spot)
    kind = jnp.where(j < 0, 0, jnp.where((j < M0) & jnp.logical_not(full), 2, 1))
    spot = jnp.where(kind == 2, j, spot)
    table(5, spot, HALF + SPREAD - 1)
    table(6, kind, 2)
    table(7, j, HALF - 1)


def move_kernel(ends, tables, weights, early, staged, up, held, back, *rest):
    outs, gots = rest[:4], rest[4:8]
    ls, zs, zr, gs, gr = rest[8:]
    starts = (0,) + ends[:3]
    row, col = place()
    mate = at(across(row), col)
    peers = [neighbour(k, row, col) for k in range(9)]
    load = pltpu.make_async_copy(weights.at[pl.ds(HALF, HALF)], up, ls.at[0])
    load.start()
    load_early = pltpu.make_async_copy(early, held, ls.at[1])
    load_early.start()
    greet(peers + [mate])
    load_early.wait()
    load.wait()
    zs_all = [send(outs[i], gots[i], zs.at[i], zr.at[i], mate) for i in range(4)]
    for part in range(4):
        start, target = starts[part], outs[part]

        @pl.loop(0, ends[part] - start)
        def _(i):
            t = start + i
            target[i] = jnp.where(tables[3, t] == 1, held[tables[2, t]], up[tables[1, t]])

        zs_all[part].start()

    def received(t, parts):
        value = gots[0][jnp.minimum(t, ends[0] - 1)]
        for p in range(1, parts):
            size = ends[p] - starts[p]
            value = jnp.where(t < starts[p], value, gots[p][jnp.clip(t - starts[p], 0, size - 1)])
        return value

    waits, stores = [], []
    for part in range(4):
        zs_all[part].wait_recv()
        for i, (k, n, base) in enumerate(RANGES):
            if i // 8 != part:
                continue

            @pl.loop(base, base + n)
            def _(slot):
                back[slot] = received(tables[4, slot], part + 1)

            there = RANGES[BACK[i]][2]
            send(
                back.at[pl.ds(base, n)], staged.at[pl.ds(HALF + there, n)], gs.at[i], gr.at[BACK[i]], peers[k]
            ).start()
            waits.append(send(back.at[pl.ds(base, n)], staged.at[pl.ds(HALF + base, n)], gs.at[i], gr.at[i], peers[k]))
        store = pltpu.make_async_copy(
            gots[part], staged.at[pl.ds(starts[part], ends[part] - starts[part])], ls.at[2 + part]
        )
        store.start()
        stores.append(store)
    for store in stores:
        store.wait()
    for copy in zs_all:
        copy.wait_send()
    for come in waits:
        come.wait()


def full_kernel(weights, staged, ss, rs):
    row, col = place()
    mate = at(across(row), col)
    greet([mate])
    copy = send(weights.at[pl.ds(HALF, HALF)], staged.at[pl.ds(0, HALF)], ss, rs, mate)
    copy.start()
    copy.wait()


STAGED = jax.ShapeDtypeStruct((HALF + SPREAD, G, G), F32)


def move(index, tables, weights, early):
    dma = pltpu.SemaphoreType.DMA
    if index == len(RUNGS):
        return pl.pallas_call(
            full_kernel,
            out_shape=STAGED,
            in_specs=[ANY],
            out_specs=ANY,
            scratch_shapes=[dma, dma],
            compiler_params=pltpu.CompilerParams(
                collective_id=2 + index, has_side_effects=True, vmem_limit_bytes=VMEM_LIMIT
            ),
            name="move_full",
        )(weights)
    ends = RUNGS[index]

    def blocks(n):
        return pltpu.VMEM((n, G, G), F32)

    parts = [blocks(b - a) for a, b in zip((0,) + ends[:3], ends)]
    return pl.pallas_call(
        functools.partial(move_kernel, ends),
        out_shape=STAGED,
        in_specs=[SMEM, ANY, ANY],
        out_specs=ANY,
        scratch_shapes=[
            blocks(HALF), blocks(SPREAD), blocks(SPREAD), *parts, *parts,
            dma((6,)), dma((4,)), dma((4,)), dma((17,)), dma((17,)),
        ],
        compiler_params=pltpu.CompilerParams(
            collective_id=2 + index, has_side_effects=True, vmem_limit_bytes=VMEM_LIMIT
        ),
        name=f"move_{ends[3]}",
    )(tables, weights, early)


CHUNK = 8
KP = 64


def split(value):
    high = value.astype(BF16)
    return high, (value - high.astype(F32)).astype(BF16)


def blocks_kernel(
    tables, pre, post, pidx, tab, rtab, ptab, weights, staged, z0, new, cur, qs, ds, ps, scr, acc, win, wout, sem_in, sem_out
):
    steps = HALF // CHUNK

    @pl.loop(0, HALF, unroll=4)
    def _(s):
        kind, spot, arrived = tables[6, s], tables[5, s], sem_in.at[s // CHUNK]

        @pl.when(kind == 0)
        def _():
            pltpu.make_async_copy(weights.at[s], win.at[s], arrived).start()

        @pl.when(kind == 1)
        def _():
            pltpu.make_async_copy(staged.at[spot], win.at[s], arrived).start()

        @pl.when(kind == 2)
        def _():
            pltpu.make_async_copy(z0.at[jnp.minimum(spot, M0 - 1)], win.at[s], arrived).start()

    neuron = lax.broadcasted_iota(I32, (1, G), 1)
    lane = lax.broadcasted_iota(I32, (G, G), 1)
    polarity = jnp.where(lax.rem(neuron, 5) == 4, -INHIB_GAIN, 1.0).astype(F32)

    use, supply, fast = tab[:, 10, :], tab[:, 11, :], tab[:, 12, :]
    scr[...] = jnp.zeros_like(scr)
    for t in range(STEPS):
        s = tab[:, t, :]
        use = BASE_USE + (use - BASE_USE) * USE_DECAY
        use = use + s * BASE_USE * (1.0 - use)
        release = s * use * supply
        supply = supply + SUPPLY_RATE * (1.0 - supply) - release
        fast = fast * PLUS_DECAY + s
        scr[:, t, :] = fast
        scr[:, STEPS + t, :] = release

    @pl.loop(0, ROWS, unroll=8)
    def _(g):
        terms = scr[g]
        high = terms.astype(BF16).astype(F32)
        low = terms - high
        qs[g] = jnp.concatenate([high[:20], low[:20], high[:20], jnp.zeros((4, G), F32)], axis=0).astype(BF16)
        driven = terms[STEPS : 2 * STEPS] * polarity
        dh = driven.astype(BF16).astype(F32)
        dl = driven - dh
        pad6 = jnp.zeros((6, G), F32)
        wide = jnp.concatenate([dh, pad6, dl, pad6, jnp.zeros((G - 32, G), F32)], axis=0)
        tall = jnp.transpose(wide)
        only = jnp.where(lane < 16, tall, 0.0)
        ds[g, pl.ds(0, G), :] = tall.astype(BF16)
        ds[g, pl.ds(G, G), :] = only.astype(BF16)

    for half, source in enumerate((rtab, ptab)):
        fast_p, slow_p = source[:, 13, :], source[:, 14, :]
        for t in range(STEPS):
            s = source[:, t, :]
            scr[pl.ds(half * COLS, COLS), t, :] = s * (PAIR_UP + TRIPLET_UP * slow_p)
            scr[pl.ds(half * COLS, COLS), STEPS + t, :] = -(PAIR_DOWN * fast_p)
            fast_p = fast_p * MINUS_DECAY + s
            slow_p = slow_p * SLOW_DECAY + s

    @pl.loop(0, 2 * COLS, unroll=8)
    def _(g):
        terms = scr[g] * LEARN_RATE
        high = terms.astype(BF16).astype(F32)
        low = terms - high
        rows = jnp.concatenate([high[:20], high[:20], low[:20], jnp.zeros((G - 60, G), F32)], axis=0)
        ps[g] = jnp.transpose(rows).astype(BF16)

    acc[...] = jnp.zeros_like(acc)

    @pl.loop(0, steps)
    def _(step):
        chunk = pl.ds(step * CHUNK, CHUNK)
        pltpu.make_async_copy(weights.at[pl.ds(0, CHUNK)], win.at[chunk], sem_in.at[step]).wait()
        currents = []
        for b in range(CHUNK):
            s = step * CHUNK + b
            moved, there = tables[6, s] >= 1, tables[7, s]
            p = jnp.where(moved, pidx[0, there], pre[s])
            q = jnp.where(moved, pidx[1, there] + COLS, post[s])
            w = win[s]
            change = jnp.dot(ps[q][:, :KP], qs[p], preferred_element_type=F32)
            wh, wl = split(w)
            currents.append((q, jnp.dot(jnp.concatenate([wh, wl], axis=1), ds[p], preferred_element_type=F32)))
            wout[s] = jnp.clip(w + change, 0.0, WEIGHT_MAX)
        for q, value in currents:
            acc[q] += value
        pltpu.make_async_copy(wout.at[chunk], new.at[chunk], sem_out).start()

    for q in range(2 * COLS):
        turned = jnp.transpose(acc[q])
        cur[q] = turned[0:16] + turned[16:32]
    pltpu.make_async_copy(wout, new, sem_out).wait()


def do_blocks(tables, pre, post, pidx, tab, rtab, ptab, weights, staged, z0):
    dma = pltpu.SemaphoreType.DMA
    return pl.pallas_call(
        blocks_kernel,
        out_shape=(jax.ShapeDtypeStruct((HALF, G, G), F32), jax.ShapeDtypeStruct((2 * COLS, 16, G), F32)),
        in_specs=[SMEM, SMEM, SMEM, SMEM, VMEM, VMEM, VMEM, ANY, ANY, ANY],
        out_specs=(ANY, VMEM),
        scratch_shapes=[
            pltpu.VMEM((ROWS, KP, G), BF16),
            pltpu.VMEM((ROWS, 2 * G, G), BF16),
            pltpu.VMEM((2 * COLS, G, G), BF16),
            pltpu.VMEM((ROWS, 24, G), F32),
            pltpu.VMEM((2 * COLS, G, G), F32),
            pltpu.VMEM((HALF, G, G), F32),
            pltpu.VMEM((HALF, G, G), F32),
            dma((HALF // CHUNK,)), dma,
        ],
        compiler_params=pltpu.CompilerParams(vmem_limit_bytes=VMEM_LIMIT),
        name="blocks",
    )(tables, pre, post, pidx, tab, rtab, ptab, weights, staged, z0)


def currents_kernel(cur, out, got, ss, rs):
    row, col = place()
    far = across(row)
    peers, copies, arrivals = [], [], []
    for d in range(1, COLS):
        c = lax.rem(col + d, COLS)
        peers.append(at(row, c))
        copies.append(send(cur.at[c], got.at[col], ss.at[d], rs.at[col], at(row, c)))
        arrivals.append(send(cur.at[c], got.at[c], ss.at[d], rs.at[c], at(row, c)))
    for d in range(COLS):
        c = lax.rem(col + d, COLS)
        peers.append(at(far, c))
        copies.append(send(cur.at[COLS + c], got.at[COLS + col], ss.at[COLS + d], rs.at[COLS + col], at(far, c)))
        arrivals.append(send(cur.at[COLS + c], got.at[COLS + c], ss.at[COLS + d], rs.at[COLS + c], at(far, c)))
    greet(peers)
    for copy in copies:
        copy.start()
    got[col] = cur[col]
    for copy in arrivals:
        copy.wait()
    drive = got[0]
    for i in range(1, 2 * COLS):
        drive = drive + got[i]
    gain = 1.0 / math.sqrt(G * HALF)
    state = jnp.zeros((1, G), F32)
    for t in range(STEPS):
        state = state * SYN_DECAY + gain * drive[t : t + 1]
        out[pl.ds(t, 1), :] = state


def settle(cur):
    dma = pltpu.SemaphoreType.DMA
    return pl.pallas_call(
        currents_kernel,
        out_shape=jax.ShapeDtypeStruct((STEPS, G), F32),
        in_specs=[VMEM],
        out_specs=VMEM,
        scratch_shapes=[pltpu.VMEM((2 * COLS, 16, G), F32), dma((2 * COLS,)), dma((2 * COLS,))],
        compiler_params=pltpu.CompilerParams(collective_id=1, has_side_effects=True),
        name="currents",
    )(cur)


def body(spikes, stp_init, trace_init, weights, block_pre, block_post, block_count):
    own = weights[0, 0]
    pre, post = block_pre[0, 0], block_post[0, 0]
    tab, rtab, ptab, pidx, tables, rung, z0, early = first(
        spikes, stp_init, trace_init, block_count, pre.reshape(2, G), post.reshape(2, G), own
    )
    staged = lax.switch(
        rung[0], [functools.partial(move, i) for i in range(len(RUNGS) + 1)], tables, own, early
    )
    new, cur = do_blocks(tables, pre, post, pidx, tab, rtab, ptab, own, staged, z0)
    synaptic = settle(cur)
    return (new[None, None], synaptic)


def solution(mesh):
    placed = (
        P(None, ("row", "col")),
        P(None, ("row", "col")),
        P(None, ("row", "col")),
        P("row", "col", None, None, None),
        P("row", "col", None),
        P("row", "col", None),
        P("row", "col"),
    )
    return jax.shard_map(
        body,
        mesh=mesh,
        in_specs=placed,
        out_specs=(P("row", "col", None, None, None), P(None, ("row", "col"))),
        check_vma=False,
    )
```

```python
import functools
import math

import jax
import jax.numpy as jnp
from jax import lax
from jax.experimental import pallas as pl
from jax.experimental.pallas import tpu as pltpu
from jax.sharding import PartitionSpec as P

BASE_USE = 0.25
USE_DECAY = 0.98
SUPPLY_RATE = 0.005
PLUS_DECAY = math.exp(-1.0 / 16.8)
MINUS_DECAY = math.exp(-1.0 / 33.7)
SLOW_DECAY = math.exp(-1.0 / 114.0)
SYN_DECAY = math.exp(-1.0 / 5.0)
PAIR_UP = 1.0
TRIPLET_UP = 0.8
PAIR_DOWN = 0.9
LEARN_RATE = 0.02
WEIGHT_MAX = 1.0
INHIB_GAIN = 4.0

G = 128
HALF = 128
STEPS = 10
ROWS = 32
COLS = 4
MESH = pl.DeviceIdType.MESH
F32 = jnp.float32
I32 = jnp.int32
BF16 = jnp.bfloat16

EA = 4
EB = 3
ES = 32
M0 = 16
RUNGS = ((16, 22, 28, 30), (16, 23, 29, 32), (17, 25, 31, 35), (20, 32, 40, 44))
M0_FIRST = 6
ITERS = 12
STEP_W = 10.0
INVERSE = (0, 3, 4, 1, 2, 7, 8, 5, 6)
RANGES = tuple(
    [(k, EA, (k - 1) * EA) for k in range(1, 9)]
    + [(k, EB, 8 * EA + (k - 1) * EB) for k in range(1, 9)]
    + [(0, ES, 8 * (EA + EB))]
)
BACK = tuple([INVERSE[k] - 1 for k in range(1, 9)] + [7 + INVERSE[k] for k in range(1, 9)] + [16])
SPREAD = 8 * (EA + EB) + ES
VMEM_LIMIT = 60 * 1024 * 1024
ANY = pl.BlockSpec(memory_space=pl.ANY)
SMEM = pl.BlockSpec(memory_space=pltpu.SMEM)
VMEM = pl.BlockSpec(memory_space=pltpu.VMEM)


def place():
    row, col = lax.axis_index("row"), lax.axis_index("col")
    return row, col


def at(row, col):
    return {"row": row, "col": col}


def flip_core(row):
    return row + 1 - 2 * lax.rem(row, 2)


def across(row):
    return lax.rem(row + ROWS // 2, ROWS)


def shift_x(row, step):
    within = lax.rem(row, 8)
    return row - within + lax.rem(within + 2 * step + 8, 8)


def neighbour(k, row, col):
    if k == 0:
        return at(flip_core(row), col)
    which, other = (k - 1) // 2, (k - 1) % 2
    if which < 2:
        row = shift_x(row, 1 if which == 0 else -1)
    else:
        col = lax.rem(col + (1 if which == 2 else COLS - 1), COLS)
    return at(flip_core(row) if other else row, col)


def greet(peers):
    barrier = pltpu.get_barrier_semaphore()
    for peer in peers:
        pl.semaphore_signal(barrier, inc=1, device_id=peer, device_id_type=MESH)
    pl.semaphore_wait(barrier, len(peers))


def send(src, dst, send_sem, recv_sem, peer):
    return pltpu.make_async_remote_copy(
        src_ref=src, dst_ref=dst, send_sem=send_sem, recv_sem=recv_sem, device_id=peer, device_id_type=MESH
    )


def first_kernel(
    spikes, stp, trace, held, pre, post, weights,
    tab, rtab, ptab, pidx, tables, rung, z0, early,
    pack, idx, cnt, s1, r1, s2, r2, s3, r3, s4, r4, s5, r5, s6, r6, s7, r7, s8, r8,
):
    row, col = place()
    far = across(row)
    mate = at(far, col)
    barrier = pltpu.get_barrier_semaphore()

    plane, within = row // 8, lax.rem(row, 8)

    def in_plane(d):
        return plane * 8 + lax.rem(within + d, 8)

    for d in range(1, 8):
        pl.semaphore_signal(barrier, inc=1, device_id=at(in_plane(d), col), device_id_type=MESH)
    for d in range(1, 4):
        pl.semaphore_signal(barrier, inc=1, device_id=at(lax.rem(row + 8 * d, ROWS), col), device_id_type=MESH)
    for d in range(1, COLS):
        c = lax.rem(col + d, COLS)
        pl.semaphore_signal(barrier, inc=1, device_id=at(row, c), device_id_type=MESH)
        pl.semaphore_signal(barrier, inc=1, device_id=at(far, c), device_id_type=MESH)
    for k in (6, 8):
        pl.semaphore_signal(barrier, inc=1, device_id=neighbour(k, row, col), device_id_type=MESH)

    count_row = jnp.broadcast_to(held[...].astype(F32), (1, G))
    pack[pl.ds(0, STEPS), :] = spikes[...].astype(F32)
    pack[pl.ds(10, 2), :] = stp[...]
    pack[pl.ds(12, 3), :] = trace[...]
    pack[pl.ds(15, 1), :] = count_row
    idx[...] = jnp.concatenate([pre[pl.ds(1, 1), :], post[pl.ds(1, 1), :], jnp.zeros((6, G), I32)], axis=0)
    cnt[row, col] = count_row
    tab[row] = pack[...]
    rtab[col] = pack[...]
    pl.semaphore_wait(barrier, 7 + 3 + 2 * (COLS - 1) + 2)

    for d in range(1, COLS):
        c = lax.rem(col + d, COLS)
        send(cnt.at[row, col], cnt.at[row, col], s4.at[d], r4.at[1 + col], at(row, c)).start()
    z_parts = [
        send(weights.at[pl.ds(HALF + a, n)], z0.at[pl.ds(a, n)], s6.at[17 + i], r6.at[17 + i], mate)
        for i, (a, n) in enumerate(((0, M0_FIRST), (M0_FIRST, M0 - M0_FIRST)))
    ]
    z_parts[0].start()
    ahead = []
    for i, (k, n, base) in enumerate(RANGES):
        there = RANGES[BACK[i]][2]
        ahead.append(
            send(
                weights.at[pl.ds(HALF + M0 + base, n)], early.at[pl.ds(there, n)],
                s6.at[i], r6.at[BACK[i]], neighbour(k, row, col),
            )
        )
    along_y = [copy for copy, (k, _, _) in zip(ahead, RANGES) if k > 4]
    others = [copy for copy, (k, _, _) in zip(ahead, RANGES) if k <= 4]
    for d in range(1, COLS):
        c = lax.rem(col + d, COLS)
        send(pack, rtab.at[col], s2.at[d], r2.at[col], at(row, c)).start()
    for copy in along_y:
        copy.start()
    for d in range(1, COLS):
        c = lax.rem(col + d, COLS)
        send(cnt.at[row, c], cnt.at[row, c], s4.at[d], r4.at[1 + c], at(row, c)).wait()

    for d in range(1, 8):
        send(cnt.at[row], cnt.at[row], s5.at[d], r5.at[within], at(in_plane(d), col)).start()
    for d in range(1, 8):
        send(pack, tab.at[row], s1.at[d], r1.at[within], at(in_plane(d), col)).start()
    for copy in others:
        copy.start()
    for d in range(1, 8):
        source = in_plane(d)
        send(cnt.at[source], cnt.at[source], s5.at[d], r5.at[lax.rem(within + d, 8)], at(source, col)).wait()
    ours = pl.ds(plane * 8, 8)
    for d in range(1, 4):
        peer = at(lax.rem(row + 8 * d, ROWS), col)
        send(cnt.at[ours], cnt.at[ours], s7.at[d], r7.at[plane], peer).start()
    for d in range(COLS):
        c = lax.rem(col + d, COLS)
        send(pack, ptab.at[col], s3.at[d], r3.at[col], at(far, c)).start()
    last = send(idx, pidx, s4.at[0], r4.at[0], mate)
    last.start()
    for d in range(1, 8):
        source = in_plane(d)
        send(pack, tab.at[source], s1.at[d], r1.at[lax.rem(within + d, 8)], at(source, col)).wait()
    for d in range(1, 4):
        peer = at(lax.rem(row + 8 * d, ROWS), col)
        send(tab.at[ours], tab.at[ours], s8.at[d], r8.at[plane], peer).start()
    z_parts[1].start()
    for d in range(1, 4):
        p = lax.rem(plane + d, 4)
        theirs = pl.ds(p * 8, 8)
        send(cnt.at[theirs], cnt.at[theirs], s7.at[d], r7.at[p], at(lax.rem(row + 8 * d, ROWS), col)).wait()

    make_plan(row, col, cnt, tables, rung)

    for d in range(1, 4):
        p = lax.rem(plane + d, 4)
        theirs = pl.ds(p * 8, 8)
        send(tab.at[theirs], tab.at[theirs], s8.at[d], r8.at[p], at(lax.rem(row + 8 * d, ROWS), col)).wait()
    for d in range(1, COLS):
        c = lax.rem(col + d, COLS)
        send(pack, rtab.at[c], s2.at[d], r2.at[c], at(row, c)).wait()
    for d in range(COLS):
        c = lax.rem(col + d, COLS)
        send(pack, ptab.at[c], s3.at[d], r3.at[c], at(far, c)).wait()
    last.wait()
    for part in z_parts:
        part.wait()
    for i, (k, n, base) in enumerate(RANGES):
        send(
            weights.at[pl.ds(HALF + M0 + base, n)], early.at[pl.ds(base, n)], s6.at[i], r6.at[i], neighbour(k, row, col)
        ).wait()


def first(spikes, stp, trace, held, pre, post, weights):
    dma = pltpu.SemaphoreType.DMA
    return pl.pallas_call(
        first_kernel,
        out_shape=(
            jax.ShapeDtypeStruct((ROWS, 16, G), F32),
            jax.ShapeDtypeStruct((COLS, 16, G), F32),
            jax.ShapeDtypeStruct((COLS, 16, G), F32),
            jax.ShapeDtypeStruct((8, G), I32),
            jax.ShapeDtypeStruct((8, G), I32),
            jax.ShapeDtypeStruct((1,), I32),
            jax.ShapeDtypeStruct((M0, G, G), F32),
            jax.ShapeDtypeStruct((SPREAD, G, G), F32),
        ),
        in_specs=[VMEM] * 6 + [ANY],
        out_specs=(VMEM, VMEM, VMEM, VMEM, VMEM, SMEM, ANY, ANY),
        scratch_shapes=[
            pltpu.VMEM((16, G), F32), pltpu.VMEM((8, G), I32),
            pltpu.VMEM((ROWS, COLS, 1, G), F32),
            dma((8,)), dma((8,)), dma((COLS,)), dma((COLS,)), dma((COLS,)), dma((COLS,)),
            dma((COLS,)), dma((COLS + 1,)), dma((8,)), dma((8,)), dma((19,)), dma((19,)),
            dma((4,)), dma((4,)), dma((4,)), dma((4,)),
        ],
        compiler_params=pltpu.CompilerParams(
            collective_id=0, has_side_effects=True, vmem_limit_bytes=VMEM_LIMIT
        ),
        name="first",
    )(spikes, stp, trace, held, pre, post, weights)


def make_plan(row, col, cnt, tables, rung):
    shape = (8, G)
    lane = lax.broadcasted_iota(I32, shape, 1)
    slot = lax.broadcasted_iota(I32, (1, G), 1)

    def pick(r, total):
        for c in range(COLS):
            total = jnp.where(slot == c * ROWS + r, cnt[r, c], total)
        return total

    total = lax.fori_loop(0, ROWS, pick, jnp.zeros((1, G), F32))
    count = jnp.broadcast_to(total, shape)
    surplus = jnp.maximum(count - HALF, 0.0)
    core = lax.rem(lane, 2)
    x_at = lax.rem(lane, 8) // 2
    z_hi = lax.rem(lane, 32) // 16

    def roll(value, by):
        return pltpu.roll(value, by % G, 1)

    def from_sibling(v):
        return jnp.where(core == 0, roll(v, -1), roll(v, 1))

    def seen(v):
        same = (
            jnp.where(x_at == 3, roll(v, 6), roll(v, -2)),
            jnp.where(x_at == 0, roll(v, -6), roll(v, 2)),
            roll(v, -ROWS),
            roll(v, ROWS),
        )
        out = [from_sibling(v)]
        for value in same:
            out += [value, from_sibling(value)]
        return out

    def toward(which, v):
        if which == 0:
            return jnp.where(x_at == 3, roll(v, 6), roll(v, -2))
        if which == 1:
            return jnp.where(x_at == 0, roll(v, -6), roll(v, 2))
        return roll(v, -ROWS if which == 2 else ROWS)

    def arriving(v):
        out = [from_sibling(v[0])]
        for k in range(1, 9):
            value = toward((k - 1) // 2, v[INVERSE[k]])
            out.append(from_sibling(value) if (k - 1) % 2 else value)
        return out

    def add(values):
        return functools.reduce(jnp.add, values)

    zero = jnp.zeros(shape, F32)
    free = jnp.maximum(surplus - M0, 0.0)
    tops = [jnp.clip(surplus - float(M0 + base), 0.0, float(n)) for _, n, base in RANGES]
    top_a = [zero] + tops[:8]
    top = [tops[16]] + [tops[i] + tops[8 + i] for i in range(8)]
    outs, ins = [zero] * 9, [zero] * 9
    for _ in range(ITERS):
        load = jnp.maximum(surplus - add(outs), float(M0)) + add(ins)
        near = seen(load)
        outs = [jnp.clip(outs[k] + (load - near[k]) * (1.0 / STEP_W), 0.0, top[k]) for k in range(9)]
        scale = jnp.minimum(1.0, free / jnp.maximum(add(outs), 1e-6))
        outs = [v * scale for v in outs]
        ins = arriving(outs)
    give = [jnp.minimum(jnp.floor(v + 0.5), top[k]) for k, v in enumerate(outs)]
    over = jnp.maximum(add(give) - free, 0.0)
    for k in range(9):
        less = jnp.minimum(give[k], over)
        give[k] = give[k] - less
        over = over - less
    give_a = [jnp.minimum(give[k], top_a[k]) for k in range(9)]
    give_b = [give[k] - give_a[k] for k in range(9)]
    take_a, take_b = arriving(give_a), arriving(give_b)
    gives = give_a[1:] + give_b[1:] + give_b[:1]
    takes = take_a[1:] + take_b[1:] + take_b[:1]
    lefts = [tops[i] - gives[i] for i in range(17)]
    in_a = add(takes[:8])
    in_ab = in_a + add(takes[8:16])
    in_all = in_ab + takes[16]
    most = [jnp.max(v) for v in (in_a, in_ab, in_all, in_all + free - add(give))]
    picked = jnp.int32(len(RUNGS))
    for i in reversed(range(len(RUNGS))):
        fits = functools.reduce(jnp.logical_and, [m <= float(n) for m, n in zip(most, RUNGS[i])])
        picked = jnp.where(fits, i, picked)
    full = picked == len(RUNGS)
    rung[0] = picked

    me = col * ROWS + row
    mate = col * ROWS + across(row)

    def of(v, who):
        return jnp.max(jnp.where(lane == who, v, -1.0), axis=1, keepdims=True).astype(I32)[:1]

    def table(i, value, most):
        tables[pl.ds(i, 1), :] = jnp.clip(value, 0, most)

    none = jnp.zeros((1, 1), I32)
    held = of(count, me)
    give_me = [of(v, me) for v in gives]
    left_me = [of(v, me) for v in lefts]
    in_me = of(in_all, me)
    r = slot - in_me
    j = M0 + SPREAD + r - add(left_me)
    before = none
    for i, (_, _, base) in enumerate(RANGES):
        here = (r >= before) & (r < before + left_me[i])
        j = jnp.where(here, M0 + base + give_me[i] + r - before, j)
        before = before + left_me[i]
    table(1, j, HALF - 1)
    source = jnp.zeros((1, G), I32)
    kind = jnp.zeros((1, G), I32)
    gather = jnp.zeros((1, G), I32)
    before, ahead = none, none
    for i, (_, n, base) in enumerate(RANGES):
        amount = of(takes[i], me)
        here = (slot >= before) & (slot < before + amount)
        source = jnp.where(here, base + slot - before, source)
        kind = jnp.where(here, 1, kind)
        before = before + amount
        here = (slot >= base) & (slot < base + n)
        gather = jnp.where(here, slot - base + ahead, gather)
        ahead = ahead + of(takes[i], mate)
    table(2, source, SPREAD - 1)
    table(3, kind, 1)
    table(4, gather, HALF - 1)
    table(0, slot, HALF - 1)
    j = slot - held
    left = none
    r = jnp.zeros((1, G), I32)
    passed = jnp.zeros((1, G), I32)
    for i, (_, n, base) in enumerate(RANGES):
        amount = of(gives[i], mate)
        inside = j - (M0 + base)
        here = (inside >= 0) & (inside < n)
        passed = jnp.where(here & (inside < amount), 1, passed)
        r = jnp.where(here, left + inside - amount, r)
        left = left + of(lefts[i], mate)
    r = jnp.where(j >= M0 + SPREAD, left + j - (M0 + SPREAD), r)
    spot = jnp.where(passed == 1, HALF + j - M0, of(in_all, mate) + r)
    spot = jnp.where(full, j, spot)
    kind = jnp.where(j < 0, 0, jnp.where((j < M0) & jnp.logical_not(full), 2, 1))
    spot = jnp.where(kind == 2, j, spot)
    table(5, spot, HALF + SPREAD - 1)
    table(6, kind, 2)
    table(7, j, HALF - 1)


def move_kernel(ends, tables, weights, early, staged, up, held, back, *rest):
    outs, gots = rest[:4], rest[4:8]
    ls, zs, zr, gs, gr = rest[8:]
    starts = (0,) + ends[:3]
    row, col = place()
    mate = at(across(row), col)
    peers = [neighbour(k, row, col) for k in range(9)]
    load = pltpu.make_async_copy(weights.at[pl.ds(HALF, HALF)], up, ls.at[0])
    load.start()
    load_early = pltpu.make_async_copy(early, held, ls.at[1])
    load_early.start()
    greet(peers + [mate])
    load_early.wait()
    load.wait()
    zs_all = [send(outs[i], gots[i], zs.at[i], zr.at[i], mate) for i in range(4)]
    for part in range(4):
        start, target = starts[part], outs[part]

        @pl.loop(0, ends[part] - start)
        def _(i):
            t = start + i
            target[i] = jnp.where(tables[3, t] == 1, held[tables[2, t]], up[tables[1, t]])

        zs_all[part].start()

    def received(t, parts):
        value = gots[0][jnp.minimum(t, ends[0] - 1)]
        for p in range(1, parts):
            size = ends[p] - starts[p]
            value = jnp.where(t < starts[p], value, gots[p][jnp.clip(t - starts[p], 0, size - 1)])
        return value

    waits, stores = [], []
    for part in range(4):
        zs_all[part].wait_recv()
        for i, (k, n, base) in enumerate(RANGES):
            if i // 8 != part:
                continue

            @pl.loop(base, base + n)
            def _(slot):
                back[slot] = received(tables[4, slot], part + 1)

            there = RANGES[BACK[i]][2]
            send(
                back.at[pl.ds(base, n)], staged.at[pl.ds(HALF + there, n)], gs.at[i], gr.at[BACK[i]], peers[k]
            ).start()
            waits.append(send(back.at[pl.ds(base, n)], staged.at[pl.ds(HALF + base, n)], gs.at[i], gr.at[i], peers[k]))
        store = pltpu.make_async_copy(
            gots[part], staged.at[pl.ds(starts[part], ends[part] - starts[part])], ls.at[2 + part]
        )
        store.start()
        stores.append(store)
    for store in stores:
        store.wait()
    for copy in zs_all:
        copy.wait_send()
    for come in waits:
        come.wait()


def full_kernel(weights, staged, ss, rs):
    row, col = place()
    mate = at(across(row), col)
    greet([mate])
    copy = send(weights.at[pl.ds(HALF, HALF)], staged.at[pl.ds(0, HALF)], ss, rs, mate)
    copy.start()
    copy.wait()


STAGED = jax.ShapeDtypeStruct((HALF + SPREAD, G, G), F32)


def move(index, tables, weights, early):
    dma = pltpu.SemaphoreType.DMA
    if index == len(RUNGS):
        return pl.pallas_call(
            full_kernel,
            out_shape=STAGED,
            in_specs=[ANY],
            out_specs=ANY,
            scratch_shapes=[dma, dma],
            compiler_params=pltpu.CompilerParams(
                collective_id=2 + index, has_side_effects=True, vmem_limit_bytes=VMEM_LIMIT
            ),
            name="move_full",
        )(weights)
    ends = RUNGS[index]

    def blocks(n):
        return pltpu.VMEM((n, G, G), F32)

    parts = [blocks(b - a) for a, b in zip((0,) + ends[:3], ends)]
    return pl.pallas_call(
        functools.partial(move_kernel, ends),
        out_shape=STAGED,
        in_specs=[SMEM, ANY, ANY],
        out_specs=ANY,
        scratch_shapes=[
            blocks(HALF), blocks(SPREAD), blocks(SPREAD), *parts, *parts,
            dma((6,)), dma((4,)), dma((4,)), dma((17,)), dma((17,)),
        ],
        compiler_params=pltpu.CompilerParams(
            collective_id=2 + index, has_side_effects=True, vmem_limit_bytes=VMEM_LIMIT
        ),
        name=f"move_{ends[3]}",
    )(tables, weights, early)


CHUNK = 16
KP = 64


def split(value):
    high = value.astype(BF16)
    return high, (value - high.astype(F32)).astype(BF16)


def blocks_kernel(
    tables, pre, post, pidx, tab, rtab, ptab, weights, staged, z0, new, cur, qs, ds, ps, scr, acc, win, wout, sem_in, sem_out
):
    steps = HALF // CHUNK

    @pl.loop(0, HALF, unroll=4)
    def _(s):
        kind, spot, arrived = tables[6, s], tables[5, s], sem_in.at[s // CHUNK]

        @pl.when(kind == 0)
        def _():
            pltpu.make_async_copy(weights.at[s], win.at[s], arrived).start()

        @pl.when(kind == 1)
        def _():
            pltpu.make_async_copy(staged.at[spot], win.at[s], arrived).start()

        @pl.when(kind == 2)
        def _():
            pltpu.make_async_copy(z0.at[jnp.minimum(spot, M0 - 1)], win.at[s], arrived).start()

    neuron = lax.broadcasted_iota(I32, (1, G), 1)
    lane = lax.broadcasted_iota(I32, (G, G), 1)
    polarity = jnp.where(lax.rem(neuron, 5) == 4, -INHIB_GAIN, 1.0).astype(F32)

    use, supply, fast = tab[:, 10, :], tab[:, 11, :], tab[:, 12, :]
    scr[...] = jnp.zeros_like(scr)
    for t in range(STEPS):
        s = tab[:, t, :]
        use = BASE_USE + (use - BASE_USE) * USE_DECAY
        use = use + s * BASE_USE * (1.0 - use)
        release = s * use * supply
        supply = supply + SUPPLY_RATE * (1.0 - supply) - release
        fast = fast * PLUS_DECAY + s
        scr[:, t, :] = fast
        scr[:, STEPS + t, :] = release

    @pl.loop(0, ROWS, unroll=16)
    def _(g):
        terms = scr[g]
        high = terms.astype(BF16).astype(F32)
        low = terms - high
        qs[g] = jnp.concatenate([high[:20], low[:20], high[:20], jnp.zeros((4, G), F32)], axis=0).astype(BF16)
        driven = terms[STEPS : 2 * STEPS] * polarity
        dh = driven.astype(BF16).astype(F32)
        dl = driven - dh
        pad6 = jnp.zeros((6, G), F32)
        wide = jnp.concatenate([dh, pad6, dl, pad6, jnp.zeros((G - 32, G), F32)], axis=0)
        tall = jnp.transpose(wide)
        only = jnp.where(lane < 16, tall, 0.0)
        ds[g, pl.ds(0, G), :] = tall.astype(BF16)
        ds[g, pl.ds(G, G), :] = only.astype(BF16)

    for half, source in enumerate((rtab, ptab)):
        fast_p, slow_p = source[:, 13, :], source[:, 14, :]
        for t in range(STEPS):
            s = source[:, t, :]
            scr[pl.ds(half * COLS, COLS), t, :] = s * (PAIR_UP + TRIPLET_UP * slow_p)
            scr[pl.ds(half * COLS, COLS), STEPS + t, :] = -(PAIR_DOWN * fast_p)
            fast_p = fast_p * MINUS_DECAY + s
            slow_p = slow_p * SLOW_DECAY + s

    @pl.loop(0, 2 * COLS, unroll=8)
    def _(g):
        terms = scr[g] * LEARN_RATE
        high = terms.astype(BF16).astype(F32)
        low = terms - high
        rows = jnp.concatenate([high[:20], high[:20], low[:20], jnp.zeros((G - 60, G), F32)], axis=0)
        ps[g] = jnp.transpose(rows).astype(BF16)

    acc[...] = jnp.zeros_like(acc)

    @pl.loop(0, steps)
    def _(step):
        chunk = pl.ds(step * CHUNK, CHUNK)
        pltpu.make_async_copy(weights.at[pl.ds(0, CHUNK)], win.at[chunk], sem_in.at[step]).wait()
        currents = []
        for b in range(CHUNK):
            s = step * CHUNK + b
            moved, there = tables[6, s] >= 1, tables[7, s]
            p = jnp.where(moved, pidx[0, there], pre[s])
            q = jnp.where(moved, pidx[1, there] + COLS, post[s])
            w = win[s]
            change = jnp.dot(ps[q][:, :KP], qs[p], preferred_element_type=F32)
            wh, wl = split(w)
            currents.append((q, jnp.dot(jnp.concatenate([wh, wl], axis=1), ds[p], preferred_element_type=F32)))
            wout[s] = jnp.clip(w + change, 0.0, WEIGHT_MAX)
        for q, value in currents:
            acc[q] += value
        pltpu.make_async_copy(wout.at[chunk], new.at[chunk], sem_out).start()

    for q in range(2 * COLS):
        turned = jnp.transpose(acc[q])
        cur[q] = turned[0:16] + turned[16:32]
    pltpu.make_async_copy(wout, new, sem_out).wait()


def do_blocks(tables, pre, post, pidx, tab, rtab, ptab, weights, staged, z0):
    dma = pltpu.SemaphoreType.DMA
    return pl.pallas_call(
        blocks_kernel,
        out_shape=(jax.ShapeDtypeStruct((HALF, G, G), F32), jax.ShapeDtypeStruct((2 * COLS, 16, G), F32)),
        in_specs=[SMEM, SMEM, SMEM, SMEM, VMEM, VMEM, VMEM, ANY, ANY, ANY],
        out_specs=(ANY, VMEM),
        scratch_shapes=[
            pltpu.VMEM((ROWS, KP, G), BF16),
            pltpu.VMEM((ROWS, 2 * G, G), BF16),
            pltpu.VMEM((2 * COLS, G, G), BF16),
            pltpu.VMEM((ROWS, 24, G), F32),
            pltpu.VMEM((2 * COLS, G, G), F32),
            pltpu.VMEM((HALF, G, G), F32),
            pltpu.VMEM((HALF, G, G), F32),
            dma((HALF // CHUNK,)), dma,
        ],
        compiler_params=pltpu.CompilerParams(vmem_limit_bytes=VMEM_LIMIT),
        name="blocks",
    )(tables, pre, post, pidx, tab, rtab, ptab, weights, staged, z0)


def currents_kernel(cur, out, got, ss, rs):
    row, col = place()
    far = across(row)
    peers, copies, arrivals = [], [], []
    for d in range(1, COLS):
        c = lax.rem(col + d, COLS)
        peers.append(at(row, c))
        copies.append(send(cur.at[c], got.at[col], ss.at[d], rs.at[col], at(row, c)))
        arrivals.append(send(cur.at[c], got.at[c], ss.at[d], rs.at[c], at(row, c)))
    for d in range(COLS):
        c = lax.rem(col + d, COLS)
        peers.append(at(far, c))
        copies.append(send(cur.at[COLS + c], got.at[COLS + col], ss.at[COLS + d], rs.at[COLS + col], at(far, c)))
        arrivals.append(send(cur.at[COLS + c], got.at[COLS + c], ss.at[COLS + d], rs.at[COLS + c], at(far, c)))
    greet(peers)
    for copy in copies:
        copy.start()
    got[col] = cur[col]
    for copy in arrivals:
        copy.wait()
    drive = got[0]
    for i in range(1, 2 * COLS):
        drive = drive + got[i]
    gain = 1.0 / math.sqrt(G * HALF)
    state = jnp.zeros((1, G), F32)
    for t in range(STEPS):
        state = state * SYN_DECAY + gain * drive[t : t + 1]
        out[pl.ds(t, 1), :] = state


def settle(cur):
    dma = pltpu.SemaphoreType.DMA
    return pl.pallas_call(
        currents_kernel,
        out_shape=jax.ShapeDtypeStruct((STEPS, G), F32),
        in_specs=[VMEM],
        out_specs=VMEM,
        scratch_shapes=[pltpu.VMEM((2 * COLS, 16, G), F32), dma((2 * COLS,)), dma((2 * COLS,))],
        compiler_params=pltpu.CompilerParams(collective_id=1, has_side_effects=True),
        name="currents",
    )(cur)


def body(spikes, stp_init, trace_init, weights, block_pre, block_post, block_count):
    own = weights[0, 0]
    pre, post = block_pre[0, 0], block_post[0, 0]
    tab, rtab, ptab, pidx, tables, rung, z0, early = first(
        spikes, stp_init, trace_init, block_count, pre.reshape(2, G), post.reshape(2, G), own
    )
    staged = lax.switch(
        rung[0], [functools.partial(move, i) for i in range(len(RUNGS) + 1)], tables, own, early
    )
    new, cur = do_blocks(tables, pre, post, pidx, tab, rtab, ptab, own, staged, z0)
    synaptic = settle(cur)
    return (new[None, None], synaptic)


def solution(mesh):
    placed = (
        P(None, ("row", "col")),
        P(None, ("row", "col")),
        P(None, ("row", "col")),
        P("row", "col", None, None, None),
        P("row", "col", None),
        P("row", "col", None),
        P("row", "col"),
    )
    return jax.shard_map(
        body,
        mesh=mesh,
        in_specs=placed,
        out_specs=(P("row", "col", None, None, None), P(None, ("row", "col"))),
        check_vma=False,
    )
```
